128 devices in a mesh: mkt: 32 (over x, z, core), grp: 4 (over y).
Axes of the slice: x: 4, y: 4, z: 4, core: 2. Of those that a mesh axis runs over, the one named last changes fastest.
Arguments:
- mean_utility: float32 [2048, 64], P(('mkt', 'grp')), may hold values from -5 to -1
- market_share: float32 [2048, 64], P(('mkt', 'grp')), may hold values from 0.001 to 0.02
- product_traits: float32 [2048, 64, 5], P(('mkt', 'grp')), may hold values from -1 to 1
- taste_draws: float32 [2048, 5, 1024], P(('mkt', 'grp')), may hold values from -4 to 4
- taste_scale: float32 [5], replicated, may hold values from 0.3 to 1
- type_weight: float32 [2048, 1024], P(('mkt', 'grp')), may hold values from 0.1 to 1
- market_size: float32 [2048], P(('mkt', 'grp')), may hold values from 0.05 to 3
- product_firm: int32 [2048, 64], P(('mkt', 'grp')), may hold values from 0 to 511, all different within a row
- firm_order: int32 [512], replicated, may hold values from 0 to 511, each once
- loyalty: float32 [512, 1024], P(('mkt', 'grp')), may hold values from -1 to 1
- firm_share: float32 [512, 1024], replicated, may hold values from 2e-05 to 0.15
Outputs:
- utility_out: float32 [2048, 64], P(('mkt', 'grp'))
- loyalty_out: float32 [512, 1024], P(('mkt', 'grp'))
The draws below stay inside these ranges and needn't reach their ends.
Inputs may be any that keep to these rules, and one draw needn't show every extreme that they name: `product_firm`: in each market the 64 products belong to 64 different firms, and every firm sells in some market. `firm_order`: each firm appears once.
All inputs are finite; a program needn't handle non-finite values.
Results may differ from the reference program's by a relative error of at most 0.0001.
Values sent between devices are 32-bit elements; how exact they have to be, the bound alone decides.
A program may use at most 64 MiB of HBM per device.

```python
import math
import jax
import jax.numpy as jnp
from jax import lax

J = 64
FIRMS = 512
R = 1024
K = 5
ITERS = 3
M_DEV = 16
MARKETS = 2048


def draw_market_size(key, part):
    index = jnp.arange(MARKETS, dtype=jnp.float32)
    base = 1.0 + 2.0 * index / max(MARKETS - 1, 1)
    factor = jnp.exp(jax.random.uniform(key, (MARKETS,), jnp.float32, jnp.log(0.05), 0.0))
    return base * factor


def draw_firm_share(key, part):
    key_firm = jax.random.fold_in(key, 11)
    key_type = jax.random.fold_in(key, 12)
    key_noise = jax.random.fold_in(key, 13)
    firm_level = jax.random.uniform(key_firm, (FIRMS, 1), jnp.float32, -2.5, 2.5)
    noise = jnp.clip(0.5 * jax.random.normal(key_noise, (FIRMS, R), jnp.float32), -1.0, 1.0)
    type_level = jax.random.uniform(key_type, (1, R), jnp.float32, -0.5, 0.5)
    return jnp.exp(-6.5 + firm_level + type_level + noise)


def shard_levels(stream_key, shape, cuts, low, high):
    level = 1.0
    for position, shards_of in cuts:
        draws = jax.random.uniform(jax.random.fold_in(jax.random.fold_in(stream_key, 6), position), (shards_of,), jnp.float32, low / len(cuts), high / len(cuts))
        level = level * jnp.repeat(jnp.exp(draws), shape[position] // shards_of).reshape((-1,) + (1,) * (len(shape) - 1 - position))
    return level


def distinct(own_key, rows, number_of, top, lift):
    ranking = jax.random.permutation(jax.random.fold_in(own_key, 1), number_of)
    pull = ranking
    for power in range(3):
        pull = pull * pull // number_of
    pull = pull * lift // number_of
    tickets = jax.random.randint(jax.random.fold_in(own_key, 2), (rows, number_of), 0, 4096) + pull
    fixed_rows = jax.random.permutation(jax.random.fold_in(own_key, 3), rows)[jnp.arange(number_of) % rows]
    tickets = jnp.where(jnp.arange(rows)[:, None] == fixed_rows[None, :], 1 << 14, tickets)
    score = tickets * number_of + jnp.arange(number_of)
    return lax.top_k(score.astype(jnp.int32), top)[1].astype(jnp.int32)


def scatter_about(stream_key, shape, spread, most, split=(), kind=jnp.bfloat16):
    level = shard_levels(stream_key, shape, split, -0.22, 0.18) if split else 1.0
    values = jax.random.normal(stream_key, shape, jnp.float32) * spread * level
    return jnp.minimum(jnp.maximum(values, -most), most).astype(kind)


def setup_inputs(seed: int = 0) -> dict:
    seeds = jax.random.split(jax.random.key(seed), 12)
    return {
        "mean_utility": jnp.clip(-5.0 + 4.0 * jax.random.uniform(seeds[0], (MARKETS, J), jnp.float32) ** shard_levels(seeds[0], (MARKETS, J), ((0, 128),), -0.2, 0.2), -5.0, -1.0),
        "market_share": jnp.clip(jnp.exp(math.log(0.02) - 2.9957322 * jax.random.uniform(seeds[1], (MARKETS, J), jnp.float32) ** shard_levels(seeds[1], (MARKETS, J), ((0, 128),), -0.2, 0.2)), 0.001, 0.02),
        "product_traits": jnp.clip(jax.random.uniform(seeds[2], (MARKETS, J, K), jnp.float32, -1.0, 1.0) * shard_levels(seeds[2], (MARKETS, J, K), ((0, 128),), -0.4, 0.0), -1.0, 1.0),
        "taste_draws": scatter_about(seeds[3], (MARKETS, K, R), 1.0, 4.0, ((0, 128),), jnp.float32),
        "taste_scale": jnp.clip(jnp.exp(jax.random.uniform(seeds[4], (K,), jnp.float32, math.log(0.3), math.log(1.0))), 0.3, 1.0),
        "type_weight": jnp.clip(jnp.exp(math.log(1.0) - 2.3025851 * jax.random.uniform(seeds[5], (MARKETS, R), jnp.float32) ** shard_levels(seeds[5], (MARKETS, R), ((0, 128),), -0.2, 0.2)), 0.1, 1.0),
        "market_size": draw_market_size(jax.random.fold_in(seeds[11], 71), 0),
        "product_firm": distinct(seeds[7], MARKETS, FIRMS, J, 1024),
        "firm_order": jax.random.permutation(seeds[8], FIRMS).astype(jnp.int32),
        "loyalty": jnp.clip(jax.random.uniform(seeds[9], (FIRMS, R), jnp.float32, -1.0, 1.0) * shard_levels(seeds[9], (FIRMS, R), ((0, 128),), -0.4, 0.0), -1.0, 1.0),
        "firm_share": draw_firm_share(jax.random.fold_in(seeds[11], 71), 0),
    }


clip_target = 0.5
norm_eps = 1e-06

def market_terms(mean_block, traits_block, draws_block, weight_block, size_block, firms_block, table, taste_scale):
    taste = jnp.einsum('mjk,mkr->mjr', traits_block * taste_scale, draws_block, precision=lax.Precision.HIGHEST)
    expu = jnp.exp(mean_block[:, :, None] + taste + jnp.take(table, firms_block, axis=0))
    choice_prob = expu / (1.0 + lax.optimization_barrier(jnp.sum(expu, axis=1, keepdims=True)))
    predicted = jnp.einsum('mjr,mr->mj', choice_prob, weight_block, precision=lax.Precision.HIGHEST) / lax.optimization_barrier(jnp.sum(weight_block, axis=1))[:, None]
    weighted = choice_prob * (size_block[:, None] * weight_block)[:, None, :]
    partial_value = jax.ops.segment_sum(weighted.reshape(-1, weighted.shape[2]), firms_block.reshape(-1), num_segments=table.shape[0])
    return (predicted, partial_value)

def reference(mean_utility, market_share, product_traits, taste_draws, taste_scale, type_weight, market_size, product_firm, firm_order, loyalty, firm_share):
    blocks = MARKETS // M_DEV
    table = jnp.zeros((FIRMS, R), loyalty.dtype).at[firm_order].set(loyalty)
    type_mass = lax.optimization_barrier(jnp.sum(market_size[:, None] * type_weight, axis=0))
    traits_b = product_traits.reshape(blocks, M_DEV, J, K)
    draws_b = taste_draws.reshape(blocks, M_DEV, K, R)
    weight_b = type_weight.reshape(blocks, M_DEV, R)
    size_b = market_size.reshape(blocks, M_DEV)
    firms_b = product_firm.reshape(blocks, M_DEV, J)
    mean_now = mean_utility
    for step in range(ITERS):
        mean_b = mean_now.reshape(blocks, M_DEV, J)

        def scan_block(carry, pieces):
            predicted, partial_value = market_terms(pieces[0], pieces[1], pieces[2], pieces[3], pieces[4], pieces[5], table, taste_scale)
            return (carry + partial_value, predicted)
        totals, predicted = lax.scan(scan_block, jnp.zeros((FIRMS, R), jnp.float32), (mean_b, traits_b, draws_b, weight_b, size_b, firms_b))
        gap = jnp.log(firm_share) - jnp.log(totals / type_mass[None, :])
        clip = jnp.minimum(1.0, clip_target / jnp.sqrt(jnp.mean(gap * gap) + norm_eps))
        table = table + clip * gap
        mean_now = mean_now + jnp.log(market_share) - jnp.log(predicted.reshape(MARKETS, J))
    return (mean_now, jnp.take(table, firm_order, axis=0))
```

```python
import functools

import jax
import jax.numpy as jnp
from jax import lax
from jax.experimental import pallas as pl
from jax.experimental.pallas import tpu as pltpu
from jax.sharding import Mesh
from jax.sharding import PartitionSpec as P

ITERS = 3
CLIP_TARGET = 0.5
NORM_EPS = 1e-06
AXES = ("mkt_0", "mkt_1", "mkt_2", "grp")
MESH = pl.DeviceIdType.MESH
F32 = jnp.float32
BF16 = jnp.bfloat16


def split_hi_lo(value):
    hi = value.astype(BF16)
    lo = (value - hi.astype(F32)).astype(BF16)
    return hi, lo


def kernel(
    dims,
    pk_ref,
    share_ref,
    size_ref,
    weight_ref,
    loy_ref,
    order_ref,
    order_row_ref,
    draws_hbm,
    fshare_hbm,
    mean_out,
    loy_out,
    pk,
    mass_loc,
    mass,
    draws_loc,
    draws,
    fshare,
    fs_own,
    order_col,
    loy_in,
    own_table,
    table,
    tmass_s,
    tmass_r,
    onehot,
    onehot_t,
    util,
    gath,
    weighted,
    terms,
    acc,
    part,
    rs,
    pred,
    pred_r,
    dmean,
    dmean_s,
    gap_s,
    ag,
    sq_s,
    sq_r,
    sq2_s,
    sq2_r,
    loy_s,
    loc_sem,
    send,
    recv,
):
    nx, nz, nc, ny, mdev, ntraits, firms, draws_all, own = dims
    nh = nc * ny
    ng = nx * nz
    rows = firms // ng
    mrows = mdev * 64
    x, z, c, y = (lax.axis_index(a) for a in AXES)
    g = x * nz + z
    h = c * ny + y
    hpeers = [(dc, dy) for dc in range(nc) for dy in range(ny) if (dc, dy) != (0, 0)]
    gpeers = [(dx, dz) for dx in range(nx) for dz in range(nz) if (dx, dz) != (0, 0)]

    def hdev(dc, dy):
        return lax.rem(c + dc, nc), lax.rem(y + dy, ny)

    def gdev(dx, dz):
        return lax.rem(x + dx, nx), lax.rem(z + dz, nz)

    def lanes(index):
        return pl.ds(pl.multiple_of(index * 128, 128), 128)

    started = []

    def push(stage, src, dst, device):
        copy = pltpu.make_async_remote_copy(
            src_ref=src,
            dst_ref=dst,
            send_sem=send.at[stage],
            recv_sem=recv.at[stage],
            device_id=device,
            device_id_type=MESH,
        )
        copy.start()

    def to_h(stage, src_of, dst):
        for dc, dy in hpeers:
            c2, y2 = hdev(dc, dy)
            push(stage, src_of(c2 * ny + y2), dst, (x, z, c2, y2))

    def to_g(stage, src_of, dst_of):
        for dx, dz in gpeers:
            x2, z2 = gdev(dx, dz)
            push(stage, src_of(x2 * nz + z2), dst_of(dx * nz + dz), (x2, z2, c, y))

    def arrived(stage, like):
        started.append((stage, like))
        pltpu.make_async_copy(like, like, recv.at[stage]).wait()

    local = []

    def keep(src, dst):
        copy = pltpu.make_async_copy(src, dst, loc_sem.at[len(local)])
        copy.start()
        local.append(copy)
        return copy

    get_draws = keep(draws_hbm, draws_loc)
    get_share = keep(fshare_hbm.at[:, lanes(h)], fshare)

    barrier = pltpu.get_barrier_semaphore()
    for dc, dy in hpeers:
        c2, y2 = hdev(dc, dy)
        pl.semaphore_signal(barrier, inc=1, device_id=(x, z, c2, y2), device_id_type=MESH)
    for dx, dz in gpeers:
        x2, z2 = gdev(dx, dz)
        pl.semaphore_signal(barrier, inc=1, device_id=(x2, z2, c, y), device_id_type=MESH)

    mass_all = weight_ref[...] * size_ref[...]
    mass_loc[...] = mass_all
    row_mass = jnp.sum(mass_all, axis=1, keepdims=True)
    lane_market = lax.broadcasted_iota(jnp.int32, (mdev, 128), 1) // 8
    market = lax.broadcasted_iota(jnp.int32, (mdev, 128), 0)
    denom = jnp.sum(jnp.where(lane_market == market, row_mass, 0.0), axis=0, keepdims=True)
    for b in range(firms // 128):
        row = order_row_ref[:, b * 128 : (b + 1) * 128]
        order_col[b * 128 : (b + 1) * 128, :] = jnp.broadcast_to(row, (128, 128)).T

    pl.semaphore_wait(barrier, len(hpeers) + len(gpeers))

    to_h(0, lambda h2: pk_ref, pk.at[h])
    keep_pk = keep(pk_ref, pk.at[h])
    to_h(1, lambda h2: loy_ref.at[:, lanes(h2)], loy_in.at[h])
    keep_loy = keep(loy_ref.at[:, lanes(h)], loy_in.at[h])
    to_h(2, lambda h2: mass_loc.at[:, lanes(h2)], mass.at[h])
    keep_mass = keep(mass_loc.at[:, lanes(h)], mass.at[h])
    get_draws.wait()
    to_h(3, lambda h2: draws_loc.at[:, :, lanes(h2)], draws.at[h])
    keep_draws = keep(draws_loc.at[:, :, lanes(h)], draws.at[h])

    get_share.wait()
    for k in range(rows):
        fs_own[k : k + 1, :] = fshare[pl.ds(order_ref[g * rows + k], 1), :]
    fs_own[...] = jnp.log(fs_own[...])

    keep_pk.wait()
    arrived(0, pk.at[pl.ds(0, nh - 1)])

    def build(hh, carry):
        ids = pk[hh, ntraits + 1]
        ids_rows = pk[hh, ntraits + 2]
        order_row = order_row_ref[...]
        for b in range(mrows // 16):
            col = jnp.concatenate([ids[:, 2 * b : 2 * b + 1], ids[:, 2 * b + 1 : 2 * b + 2]], axis=0)
            hot = jnp.where(col == order_row, 1.0, 0.0).astype(BF16)
            onehot[pl.ds(pl.multiple_of(hh * mrows + b * 16, 16), 16), :] = hot
        for p in range(mrows // 128):
            row = ids_rows[p : p + 1, :]
            hot = jnp.where(order_col[...] == row, 1.0, 0.0).astype(BF16)
            onehot_t[hh, :, p * 128 : (p + 1) * 128] = hot
        return carry

    lax.fori_loop(0, nh, build, 0)

    keep_loy.wait()
    arrived(1, loy_in.at[pl.ds(0, nh - 1)])
    for hh in range(nh):
        own_table[hh * own : (hh + 1) * own, :] = loy_in[hh]
    to_g(4, lambda g2: own_table, lambda slot: table.at[g])
    keep_own = keep(own_table, table.at[g])

    keep_mass.wait()
    arrived(2, mass.at[pl.ds(0, nh - 1)])
    tm = jnp.sum(mass[...].reshape(nh * mdev, 128), axis=0, keepdims=True)
    tmass_s[...] = jnp.broadcast_to(tm, (8, 128))
    to_g(5, lambda g2: tmass_s, lambda slot: tmass_r.at[slot])

    keep_own.wait()
    arrived(4, table.at[pl.ds(0, ng - 1)])
    keep_draws.wait()
    arrived(3, draws.at[pl.ds(0, nh - 1)])

    lane = lax.broadcasted_iota(jnp.int32, (8, 128), 1)
    mean_now = pk_ref[0]
    log_share = jnp.log(share_ref[...])
    type_mass = None
    clip = None

    for step in range(ITERS):
        source = table if step == 0 else ag.at[step - 1]
        hi, lo = split_hi_lo(source[...].reshape(firms, 128))
        terms[:, :128] = hi
        terms[:, 128:] = lo

        def market_block(hh, carry, step=step, clip=clip):
            base = pl.multiple_of(hh * mrows, mrows)
            gath[...] = jnp.dot(
                onehot[pl.ds(base, mrows), :], terms[...], preferred_element_type=F32
            )
            compact = jnp.zeros((8, 128), F32)
            if step == 0:
                cols = [pk[hh, k] for k in range(ntraits + 1)]
            else:
                cols = [dmean[step - 1, hh]]
            for m in range(mdev):
                expu = []
                total = None
                if step == 0:
                    shocks = draws[hh, m]
                for jb in range(8):
                    at = m * 64 + jb * 8
                    lane_at = m * 8 + jb
                    moved = gath[at : at + 8, :128] + gath[at : at + 8, 128:]
                    where = pl.ds(pl.multiple_of(base + at, 8), 8)
                    if step == 0:
                        u = moved + cols[0][:, lane_at : lane_at + 1]
                        for k in range(ntraits):
                            u = u + cols[k + 1][:, lane_at : lane_at + 1] * shocks[k : k + 1, :]
                    else:
                        u = util[where, :] + (clip * moved + cols[0][:, lane_at : lane_at + 1])
                    if step < ITERS - 1:
                        util[where, :] = u
                    e = jnp.exp(u)
                    expu.append(e)
                    total = e if total is None else total + e
                total = jnp.sum(total, axis=0, keepdims=True)
                scale = mass[hh, m : m + 1, :] / (1.0 + total)
                wts = []
                for jb in range(8):
                    wt = expu[jb] * scale
                    wts.append(wt)
                    red = jnp.sum(wt, axis=1, keepdims=True)
                    compact = jnp.where(lane == m * 8 + jb, red, compact)
                for jb in range(0, 8, 2):
                    at = m * 64 + jb * 8
                    hi, lo = split_hi_lo(jnp.concatenate([wts[jb], wts[jb + 1]], axis=0))
                    weighted[at : at + 16, :128] = hi
                    weighted[at : at + 16, 128:] = lo
            pred[step, hh] = compact
            new = jnp.dot(onehot_t[hh], weighted[...], preferred_element_type=F32)
            acc[...] = acc[...] + new
            return carry

        acc[...] = jnp.zeros(acc.shape, F32)
        lax.fori_loop(0, nh, market_block, 0)

        base_stage = 6 + 6 * step
        to_h(base_stage, lambda h2: pred.at[step, h2], pred_r.at[step, h])
        part[step] = (acc[:, :128] + acc[:, 128:]).reshape(ng, rows, 128)
        to_g(base_stage + 1, lambda g2: part.at[step, g2], lambda slot: rs.at[step, slot - 1])

        arrived(base_stage, pred_r.at[step, pl.ds(0, nh - 1)])
        pred_r[step, h] = pred[step, h]
        num = jnp.sum(pred_r[step], axis=0)
        delta = log_share - jnp.log(num / denom)
        mean_now = mean_now + delta
        if step < ITERS - 1:
            dmean_s[step] = delta
            dmean[step, h] = delta
            to_h(base_stage + 2, lambda h2: dmean_s.at[step], dmean.at[step, h])

        if step == 0:
            arrived(5, tmass_r.at[pl.ds(1, ng - 1)])
            type_mass = tmass_s[0:1, :]
            for slot in range(1, ng):
                type_mass = type_mass + tmass_r[slot, 0:1, :]
        arrived(base_stage + 1, rs.at[step])
        totals = part[step, g]
        for slot in range(ng - 1):
            totals = totals + rs[step, slot]
        gap = fs_own[...] - jnp.log(totals / type_mass)
        if step < ITERS - 1:
            gap_s[step] = gap
            ag[step, g] = gap
            to_g(base_stage + 3, lambda g2: gap_s.at[step], lambda slot: ag.at[step, g])
        sq = jnp.sum((gap * gap).reshape(rows // 8, 8, 128), axis=0)
        sq_s[step] = sq
        sq_r[step, h] = sq
        to_h(base_stage + 4, lambda h2: sq_s.at[step], sq_r.at[step, h])
        arrived(base_stage + 4, sq_r.at[step, pl.ds(0, nh - 1)])
        sq = jnp.sum(sq_r[step], axis=0)
        sq2_s[step] = sq
        sq2_r[step, 0] = sq
        to_g(base_stage + 5, lambda g2: sq2_s.at[step], lambda slot: sq2_r.at[step, slot])
        arrived(base_stage + 5, sq2_r.at[step, pl.ds(1, ng - 1)])
        sq = jnp.sum(jnp.sum(sq2_r[step], axis=0), axis=0, keepdims=True)
        sq = jnp.sum(sq, axis=1, keepdims=True)
        clip = jnp.minimum(
            1.0, CLIP_TARGET / jnp.sqrt(sq / (firms * draws_all) + NORM_EPS)
        )
        own_new = (own_table[...] if step == 0 else own_new) + clip * gap
        if step < ITERS - 1:
            arrived(base_stage + 3, ag.at[step, pl.ds(0, ng - 1)])
            arrived(base_stage + 2, dmean.at[step, pl.ds(0, nh - 1)])

    mean_out[...] = mean_now
    for hh in range(nh):
        loy_s[hh] = own_new[hh * own : (hh + 1) * own, :]
    last = 6 + 6 * ITERS
    to_h(last, lambda h2: loy_s.at[h2], loy_out.at[:, lanes(h)])
    keep_out = keep(loy_s.at[h], loy_out.at[:, lanes(h)])
    keep_out.wait()
    arrived(last, loy_out.at[:, pl.ds(0, 128 * (nh - 1))])
    for stage, like in started:
        pltpu.make_async_copy(like, like, send.at[stage]).wait()


def local(
    mean_utility,
    market_share,
    product_traits,
    taste_draws,
    taste_scale,
    type_weight,
    market_size,
    product_firm,
    firm_order,
    loyalty,
    firm_share,
    shape,
):
    nx, nz, nc, ny = shape
    nh, ng = nc * ny, nx * nz
    mdev, ntraits, draws_all = taste_draws.shape
    firms = firm_share.shape[0]
    own = loyalty.shape[0]
    rows = firms // ng

    def columns(array):
        return array.reshape(mdev, 8, 8).transpose(2, 0, 1).reshape(8, 128)

    ids = product_firm.astype(F32)
    traits = (product_traits * taste_scale).reshape(mdev, 8, 8, ntraits)
    traits = traits.transpose(3, 2, 0, 1).reshape(ntraits, 8, 128)
    pk = jnp.concatenate(
        [columns(mean_utility)[None], traits, columns(ids)[None], ids.reshape(1, 8, 128)], axis=0
    )
    kinds = pk.shape[0]
    dims = (nx, nz, nc, ny, mdev, ntraits, firms, draws_all, own)
    vmem = pl.BlockSpec(memory_space=pltpu.VMEM)
    anywhere = pl.BlockSpec(memory_space=pl.ANY)
    scratch = [
        ((nh, kinds, 8, 128), F32),
        ((mdev, draws_all), F32),
        ((nh, mdev, 128), F32),
        ((mdev, ntraits, draws_all), F32),
        ((nh, mdev, ntraits, 128), F32),
        ((firms, 128), F32),
        ((rows, 128), F32),
        ((firms, 128), F32),
        ((nh, own, 128), F32),
        ((rows, 128), F32),
        ((ng, rows, 128), F32),
        ((8, 128), F32),
        ((ng, 8, 128), F32),
        ((nh * mdev * 64, firms), BF16),
        ((nh, firms, mdev * 64), BF16),
        ((nh * mdev * 64, 128), F32),
        ((mdev * 64, 256), F32),
        ((mdev * 64, 256), BF16),
        ((firms, 256), BF16),
        ((firms, 256), F32),
        ((ITERS, ng, rows, 128), F32),
        ((ITERS, ng - 1, rows, 128), F32),
        ((ITERS, nh, 8, 128), F32),
        ((ITERS, nh, 8, 128), F32),
        ((ITERS - 1, nh, 8, 128), F32),
        ((ITERS - 1, 8, 128), F32),
        ((ITERS - 1, rows, 128), F32),
        ((ITERS - 1, ng, rows, 128), F32),
        ((ITERS, 8, 128), F32),
        ((ITERS, nh, 8, 128), F32),
        ((ITERS, 8, 128), F32),
        ((ITERS, ng, 8, 128), F32),
        ((nh, own, 128), F32),
    ]
    stages = 6 + 6 * ITERS + 1
    mean, loy = pl.pallas_call(
        functools.partial(kernel, dims),
        name="contraction",
        out_shape=(
            jax.ShapeDtypeStruct((8, 128), F32),
            jax.ShapeDtypeStruct((own, draws_all), F32),
        ),
        in_specs=[vmem, vmem, vmem, vmem, vmem, pl.BlockSpec(memory_space=pltpu.SMEM), vmem]
        + [anywhere, anywhere],
        out_specs=(vmem, vmem),
        scratch_shapes=[pltpu.VMEM(s, d) for s, d in scratch]
        + [
            pltpu.SemaphoreType.DMA((8,)),
            pltpu.SemaphoreType.DMA((stages,)),
            pltpu.SemaphoreType.DMA((stages,)),
        ],
        compiler_params=pltpu.CompilerParams(
            collective_id=0, has_side_effects=True, vmem_limit_bytes=60 * 1024 * 1024
        ),
    )(
        pk,
        columns(market_share),
        market_size.reshape(mdev, 1),
        type_weight,
        loyalty,
        firm_order,
        firm_order.astype(F32).reshape(1, firms),
        taste_draws,
        firm_share,
    )
    mean = mean.reshape(8, mdev, 8).transpose(1, 2, 0).reshape(mdev, 64)
    return mean, loy


def solution(mesh):
    shape = (4, 4, 2, mesh.shape["grp"])
    torus = Mesh(mesh.devices.reshape(shape), AXES)
    in_specs = (
        P(AXES, None),
        P(AXES, None),
        P(AXES, None, None),
        P(AXES, None, None),
        P(),
        P(AXES, None),
        P(AXES),
        P(AXES, None),
        P(),
        P(AXES, None),
        P(),
    )
    out_specs = (P(AXES, None), P(AXES, None))
    return jax.shard_map(
        functools.partial(local, shape=shape),
        mesh=torus,
        in_specs=in_specs,
        out_specs=out_specs,
        check_vma=False,
    )
```

```python
import functools

import jax
import jax.numpy as jnp
from jax import lax
from jax.experimental import pallas as pl
from jax.experimental.pallas import tpu as pltpu
from jax.sharding import Mesh
from jax.sharding import PartitionSpec as P

ITERS = 3
CLIP_TARGET = 0.5
NORM_EPS = 1e-06
AXES = ("mkt_0", "mkt_1", "mkt_2", "grp")
MESH = pl.DeviceIdType.MESH
F32 = jnp.float32
BF16 = jnp.bfloat16
PK, SHOCK, LOY, TABLE, TMASS, OUT, PER_STEP = 0, 1, 2, 3, 4, 5, 6
PRED, RS, DMEAN, AG, SQ_G, SQ_H = 0, 1, 2, 3, 4, 5


def split_hi_lo(value):
    hi = value.astype(BF16)
    lo = (value - hi.astype(F32)).astype(BF16)
    return hi, lo


def kernel(
    dims,
    mean_ref,
    share_ref,
    firm_ref,
    traits_ref,
    scale_ref,
    size_ref,
    weight_ref,
    loy_ref,
    order_ref,
    order_row_ref,
    draws_hbm,
    fshare_hbm,
    mean_out,
    loy_out,
    square,
    pk_own,
    pk,
    shock_own,
    shock,
    fshare,
    fs_own,
    order_row_b,
    order_col_b,
    loy_in,
    own_table,
    table,
    tmass_s,
    tmass_r,
    lane_mask,
    traits_l,
    shocks_r,
    onehot,
    onehot_t,
    util,
    gsum,
    weighted_a,
    weighted_b,
    terms,
    acc,
    part,
    rs,
    pred,
    pred_r,
    dmean,
    dmean_s,
    gap_s,
    ag,
    sq_s,
    sq_r,
    sq2_s,
    sq2_r,
    loy_s,
    loc_sem,
    send,
    recv,
    recv_pk,
    recv_shock,
):
    nx, nz, nc, ny, mdev, ntraits, firms, draws_all, own = dims
    nh = nc * ny
    ng = nx * nz
    rows = firms // ng
    mrows = mdev * 64
    x, z, c, y = (lax.axis_index(a) for a in AXES)
    g = x * nz + z
    h = c * ny + y
    dys = (0, 1, 3, 2)
    hpeers = [(i % nc, dys[i // nc]) for i in range(1, nh)]
    far = {0: 0, 1: 1, 2: 2, 3: 1}
    gpeers = [(dx, dz) for dx in range(nx) for dz in range(nz) if (dx, dz) != (0, 0)]
    gpeers.sort(key=lambda d: -far[d[0]] - far[d[1]])

    def hdev(dc, dy):
        return lax.rem(c + dc, nc), lax.rem(y + dy, ny)

    def gdev(dx, dz):
        return lax.rem(x + dx, nx), lax.rem(z + dz, nz)

    def source(i):
        q = i // nc
        dy = q + q // 2 - 2 * (q // 3)
        return lax.rem(c + lax.rem(i, nc), nc) * ny + lax.rem(y + dy, ny)

    def lanes(index):
        return pl.ds(pl.multiple_of(index * 128, 128), 128)

    started = []

    def push(stage, src, dst, device, sem=None):
        pltpu.make_async_remote_copy(
            src_ref=src,
            dst_ref=dst,
            send_sem=send.at[stage],
            recv_sem=recv.at[stage] if sem is None else sem,
            device_id=device,
            device_id_type=MESH,
        ).start()

    def to_h(stage, src_of, dst, sems=None):
        for dc, dy in hpeers:
            c2, y2 = hdev(dc, dy)
            slot = dc + nc * dys.index((ny - dy) % ny)
            sem = None if sems is None else sems.at[slot]
            push(stage, src_of(c2 * ny + y2), dst, (x, z, c2, y2), sem)

    def to_g(stage, src_of, dst_of):
        for dx, dz in gpeers:
            x2, z2 = gdev(dx, dz)
            push(stage, src_of(x2 * nz + z2), dst_of(dx * nz + dz), (x2, z2, c, y))

    def arrived(stage, like):
        started.append((stage, like))
        pltpu.make_async_copy(like, like, recv.at[stage]).wait()

    def keep(src, dst, sem):
        copy = pltpu.make_async_copy(src, dst, sem)
        copy.start()
        return copy

    get_draws = keep(draws_hbm, shock_own.at[pl.ds(0, ntraits)], loc_sem.at[0])
    get_share = keep(fshare_hbm.at[:, lanes(h)], fshare, loc_sem.at[1])

    barrier = pltpu.get_barrier_semaphore()
    for dc, dy in hpeers:
        c2, y2 = hdev(dc, dy)
        pl.semaphore_signal(barrier, inc=1, device_id=(x, z, c2, y2), device_id_type=MESH)
    for dx, dz in gpeers:
        x2, z2 = gdev(dx, dz)
        pl.semaphore_signal(barrier, inc=1, device_id=(x2, z2, c, y), device_id_type=MESH)

    lane = lax.broadcasted_iota(jnp.int32, (8, 128), 1)
    lane16 = lax.broadcasted_iota(jnp.int32, (mdev, 128), 1)
    market = lax.broadcasted_iota(jnp.int32, (mdev, 128), 0)

    square[...] = jnp.zeros(square.shape, F32)
    for k in range(ntraits):
        square[k * mdev : (k + 1) * mdev, 0:64] = traits_ref[k] * scale_ref[k]
    mean_a = mean_ref[...].astype(BF16).astype(F32)
    ids = firm_ref[...].astype(F32) - 256.0
    square[5 * mdev : 6 * mdev, 0:64] = mean_a
    square[6 * mdev : 7 * mdev, 0:64] = ids
    square[7 * mdev : 8 * mdev, 0:64] = mean_ref[...] - mean_a
    pk_own[0:64, :] = square[...].T[0:64, :]
    for p in range(mdev // 2):
        even = square[6 * mdev + 2 * p : 6 * mdev + 2 * p + 1, :]
        odd = square[6 * mdev + 2 * p + 1 : 6 * mdev + 2 * p + 2, :]
        pk_own[64 + p : 65 + p, :] = even + pltpu.roll(odd, 64, 1)

    row_mass = None
    for m in range(mdev):
        shock_own[ntraits, m : m + 1, :] = weight_ref[m : m + 1, :] * size_ref[m]
    row_mass = jnp.sum(shock_own[ntraits], axis=1, keepdims=True)
    denom = jnp.sum(
        jnp.where(lax.rem(lane16, mdev) == market, row_mass, 0.0), axis=0, keepdims=True
    )

    pl.semaphore_wait(barrier, len(hpeers) + len(gpeers))

    to_h(LOY, lambda h2: loy_ref.at[:, lanes(h2)], loy_in.at[h])
    keep_loy = keep(loy_ref.at[:, lanes(h)], loy_in.at[h], loc_sem.at[2])
    to_h(PK, lambda h2: pk_own, pk.at[h], recv_pk)
    keep(pk_own, pk.at[h], recv_pk.at[0])
    get_draws.wait()
    to_h(SHOCK, lambda h2: shock_own.at[:, :, lanes(h2)], shock.at[h], recv_shock)
    keep(shock_own.at[:, :, lanes(h)], shock.at[h], recv_shock.at[0])
    started.append((PK, pk.at[pl.ds(0, nh - 1)]))
    started.append((SHOCK, shock.at[pl.ds(0, nh - 1)]))

    square[0:mdev, 0:64] = share_ref[...]
    turned = square[...].T
    log_share = jnp.zeros((8, 128), F32)
    for jb in range(8):
        block = turned[jb * 8 : jb * 8 + 8, :]
        if jb:
            block = pltpu.roll(block, jb * mdev, 1)
        log_share = jnp.where(lane // mdev == jb, block, log_share)
    log_share = jnp.log(log_share)
    order_f = order_row_ref[...].astype(F32) - 256.0
    order_row_b[...] = jnp.broadcast_to(order_f, order_row_b.shape).astype(BF16)
    for b in range(firms // 128):
        row = order_f[:, b * 128 : (b + 1) * 128]
        order_col_b[b * 128 : (b + 1) * 128, :] = jnp.broadcast_to(row, (128, 128)).T.astype(BF16)
    lane_b = lax.rem(lax.broadcasted_iota(jnp.int32, (16, 128), 1), mdev)
    for m in range(mdev):
        lane_mask[m] = jnp.where(lane_b == m, 1.0, 0.0).astype(BF16)
    kind = lax.broadcasted_iota(jnp.int32, (256, 256), 0) // mdev
    half = lax.broadcasted_iota(jnp.int32, (256, 256), 1) // 128
    kind = lax.rem(kind, 8)
    is_mean = jnp.logical_and(jnp.logical_or(kind == 5, kind == 7), half == 0)
    shocks_r[...] = jnp.where(is_mean, 1.0, 0.0).astype(BF16)
    get_share.wait()
    for k in range(rows):
        fs_own[k : k + 1, :] = fshare[pl.ds(order_ref[g * rows + k], 1), :]
    fs_own[...] = jnp.log(fs_own[...])

    keep_loy.wait()
    arrived(LOY, loy_in.at[pl.ds(0, nh - 1)])
    for hh in range(nh):
        own_table[hh * own : (hh + 1) * own, :] = loy_in[hh]
    to_g(TABLE, lambda g2: own_table, lambda slot: table.at[g])
    keep_own = keep(own_table, table.at[g], loc_sem.at[3])

    def build(i, carry):
        hh = source(i)
        pltpu.make_async_copy(pk.at[hh], pk.at[hh], recv_pk.at[i]).wait()
        base = pl.multiple_of(hh * mrows, mrows)
        one = jnp.ones((16, 128), BF16)
        zero = jnp.zeros((16, 128), BF16)
        for m in range(mdev):
            for b in range(4):
                at = 6 * mdev + m
                low = jnp.broadcast_to(pk[hh, b * 16 : b * 16 + 8, at : at + 1], (8, 128))
                high = jnp.broadcast_to(pk[hh, b * 16 + 8 : b * 16 + 16, at : at + 1], (8, 128))
                col = jnp.concatenate([low, high], axis=0).astype(BF16)
                for t in range(firms // 128):
                    hot = jnp.where(col == order_row_b[:, t * 128 : (t + 1) * 128], one, zero)
                    where = pl.ds(pl.multiple_of(base + m * 64 + b * 16, 16), 16)
                    onehot[where, t * 128 : (t + 1) * 128] = hot
        for p in range(mdev // 2):
            row = jnp.broadcast_to(pk[hh, 64 + p : 65 + p, :], (16, 128)).astype(BF16)
            for t in range(firms // 16):
                hot = jnp.where(order_col_b[t * 16 : t * 16 + 16, :] == row, one, zero)
                onehot_t[hh, t * 16 : t * 16 + 16, p * 128 : (p + 1) * 128] = hot
        return carry

    lax.fori_loop(0, nh, build, 0)

    keep_own.wait()
    arrived(TABLE, table.at[pl.ds(0, ng - 1)])

    def set_terms(source):
        hi, lo = split_hi_lo(source[...].reshape(firms, 128))
        terms[:, :128] = hi
        terms[:, 128:] = lo

    set_terms(table)

    def first(i, carry):
        hh = source(i)
        pltpu.make_async_copy(shock.at[hh], shock.at[hh], recv_shock.at[i]).wait()
        hi, lo = split_hi_lo(shock[hh, 0:ntraits].reshape(ntraits * mdev, 128))
        for part_of in range(2):
            at = part_of * 128
            shocks_r[at : at + ntraits * mdev, :128] = hi
            shocks_r[at : at + ntraits * mdev, 128:] = lo
        hi, lo = split_hi_lo(pk[hh, 0:64, :])
        for m in range(mdev):
            mask = lane_mask[m]
            for b in range(4):
                at = m * 64 + b * 16
                traits_l[at : at + 16, :128] = hi[b * 16 : b * 16 + 16] * mask
                traits_l[at : at + 16, 128:] = lo[b * 16 : b * 16 + 16] * mask
        base = pl.multiple_of(hh * mrows, mrows)
        both = jnp.dot(
            onehot[pl.ds(base, mrows), :], terms[...], preferred_element_type=F32
        ) + jnp.dot(traits_l[...], shocks_r[...], preferred_element_type=F32)
        util[pl.ds(base, mrows), :] = both[:, :128] + both[:, 128:]
        return carry

    lax.fori_loop(0, nh, first, 0)

    tm = jnp.sum(shock[:, ntraits].reshape(nh * mdev, 128), axis=0, keepdims=True)
    tmass_s[...] = tm
    to_g(TMASS, lambda g2: tmass_s, lambda slot: tmass_r.at[slot])

    delta_sum = jnp.zeros((8, 128), F32)
    type_mass = None
    clip = None
    own_new = own_table[...]

    for step in range(ITERS):
        stage = PER_STEP + 6 * step

        if step:
            def gather(hh, carry, step=step):
                base = pl.multiple_of(hh * mrows, mrows)
                both = jnp.dot(
                    onehot[pl.ds(base, mrows), :], terms[...], preferred_element_type=F32
                )
                gsum[pl.ds(base, mrows), :] = both[:, :128] + both[:, 128:]
                cols = dmean[step - 1, hh]
                for m in range(mdev):
                    for jb in range(8):
                        where = pl.ds(pl.multiple_of(base + m * 64 + jb * 8, 8), 8)
                        at = jb * mdev + m
                        util[where, :] = util[where, :] + cols[:, at : at + 1]
                return carry

            set_terms(ag.at[step - 1])
            lax.fori_loop(0, nh, gather, 0)
            arrived(stage - 6 + SQ_H, sq2_r.at[step - 1, pl.ds(0, nh - 1)])
            sq = jnp.sum(jnp.sum(sq2_r[step - 1], axis=0), axis=1, keepdims=True)
            clip = jnp.minimum(
                1.0, CLIP_TARGET / jnp.sqrt(sq / (firms * draws_all) + NORM_EPS)
            )
            own_new = own_new + clip * gap

        def choices(hh, weighted, step=step, clip=clip):
            base = pl.multiple_of(hh * mrows, mrows)
            compact = jnp.zeros((8, 128), F32)
            for m in range(mdev):
                expu = []
                total = None
                for jb in range(8):
                    where = pl.ds(pl.multiple_of(base + m * 64 + jb * 8, 8), 8)
                    u = util[where, :]
                    if step:
                        u = u + clip * gsum[where, :]
                        if step < ITERS - 1:
                            util[where, :] = u
                    e = jnp.exp(u)
                    expu.append(e)
                    total = e if total is None else total + e
                total = jnp.sum(total, axis=0, keepdims=True)
                scale = shock[hh, ntraits, m : m + 1, :] / (1.0 + total)
                for jb in range(0, 8, 2):
                    at = m * 64 + jb * 8
                    wts = [expu[jb] * scale, expu[jb + 1] * scale]
                    for k in range(2):
                        red = jnp.sum(wts[k], axis=1, keepdims=True)
                        compact = jnp.where(lane == (jb + k) * mdev + m, red, compact)
                    hi, lo = split_hi_lo(jnp.concatenate(wts, axis=0))
                    weighted[at : at + 16, :128] = hi
                    weighted[at : at + 16, 128:] = lo
            pred[step, hh] = compact

        def collect(hh, weighted):
            acc[...] = acc[...] + jnp.dot(
                onehot_t[hh], weighted[...], preferred_element_type=F32
            )

        def two_blocks(q, carry):
            collect(jnp.maximum(2 * q - 1, 0), weighted_b)
            choices(2 * q, weighted_a)
            collect(2 * q, weighted_a)
            choices(2 * q + 1, weighted_b)
            return carry

        acc[...] = jnp.zeros(acc.shape, F32)
        weighted_b[...] = jnp.zeros(weighted_b.shape, BF16)
        lax.fori_loop(0, nh // 2, two_blocks, 0)

        to_h(stage + PRED, lambda h2: pred.at[step, h2], pred_r.at[step, h])
        last = jnp.dot(onehot_t[nh - 1], weighted_b[...], preferred_element_type=F32)
        last = acc[...] + last
        part[step] = (last[:, :128] + last[:, 128:]).reshape(ng, rows, 128)
        to_g(stage + RS, lambda g2: part.at[step, g2], lambda slot: rs.at[step, slot - 1])

        arrived(stage + PRED, pred_r.at[step, pl.ds(0, nh - 1)])
        pred_r[step, h] = pred[step, h]
        num = jnp.sum(pred_r[step], axis=0)
        delta = log_share - jnp.log(num / denom)
        delta_sum = delta_sum + delta
        if step < ITERS - 1:
            dmean_s[step] = delta
            dmean[step, h] = delta
            to_h(stage + DMEAN, lambda h2: dmean_s.at[step], dmean.at[step, h])
        if step == 0:
            arrived(TMASS, tmass_r.at[pl.ds(1, ng - 1)])
            type_mass = tmass_s[...]
            for slot in range(1, ng):
                type_mass = type_mass + tmass_r[slot]

        arrived(stage + RS, rs.at[step])
        totals = part[step, g]
        for slot in range(ng - 1):
            totals = totals + rs[step, slot]
        gap = fs_own[...] - jnp.log(totals / type_mass)
        sq = jnp.sum(gap * gap, axis=0, keepdims=True)
        sq_s[step] = sq
        sq_r[step, 0] = sq
        to_g(stage + SQ_G, lambda g2: sq_s.at[step], lambda slot: sq_r.at[step, slot])
        if step < ITERS - 1:
            gap_s[step] = gap
            ag[step, g] = gap
            to_g(stage + AG, lambda g2: gap_s.at[step], lambda slot: ag.at[step, g])
        arrived(stage + SQ_G, sq_r.at[step, pl.ds(1, ng - 1)])
        sq = jnp.sum(sq_r[step], axis=0)
        sq2_s[step] = sq
        sq2_r[step, h] = sq
        to_h(stage + SQ_H, lambda h2: sq2_s.at[step], sq2_r.at[step, h])
        if step < ITERS - 1:
            arrived(stage + DMEAN, dmean.at[step, pl.ds(0, nh - 1)])
            arrived(stage + AG, ag.at[step, pl.ds(0, ng - 1)])

    square[0:8, :] = delta_sum
    turned = square[...].T
    natural = jnp.zeros((mdev, 128), F32)
    for jb in range(8):
        block = turned[jb * mdev : (jb + 1) * mdev, :]
        if jb:
            block = pltpu.roll(block, jb * 8, 1)
        natural = jnp.where(lane16 // 8 == jb, block, natural)
    mean_out[...] = mean_ref[...] + natural[:, 0:64]
    stage = PER_STEP + 6 * (ITERS - 1)
    arrived(stage + SQ_H, sq2_r.at[ITERS - 1, pl.ds(0, nh - 1)])
    sq = jnp.sum(jnp.sum(sq2_r[ITERS - 1], axis=0), axis=1, keepdims=True)
    clip = jnp.minimum(1.0, CLIP_TARGET / jnp.sqrt(sq / (firms * draws_all) + NORM_EPS))
    own_new = own_new + clip * gap
    for hh in range(nh):
        loy_s[hh] = own_new[hh * own : (hh + 1) * own, :]
    to_h(OUT, lambda h2: loy_s.at[h2], loy_out.at[:, lanes(h)])
    keep_out = keep(loy_s.at[h], loy_out.at[:, lanes(h)], loc_sem.at[4])
    keep_out.wait()
    arrived(OUT, loy_out.at[:, pl.ds(0, 128 * (nh - 1))])
    for stage, like in started:
        pltpu.make_async_copy(like, like, send.at[stage]).wait()


def local(
    mean_utility,
    market_share,
    product_traits,
    taste_draws,
    taste_scale,
    type_weight,
    market_size,
    product_firm,
    firm_order,
    loyalty,
    firm_share,
    shape,
):
    nx, nz, nc, ny = shape
    nh, ng = nc * ny, nx * nz
    mdev, ntraits, draws_all = taste_draws.shape
    firms = firm_share.shape[0]
    own = loyalty.shape[0]
    rows = firms // ng
    dims = (nx, nz, nc, ny, mdev, ntraits, firms, draws_all, own)
    vmem = pl.BlockSpec(memory_space=pltpu.VMEM)
    smem = pl.BlockSpec(memory_space=pltpu.SMEM)
    anywhere = pl.BlockSpec(memory_space=pl.ANY)
    scratch = [
        ((128, 128), F32),
        ((72, 128), F32),
        ((nh, 72, 128), F32),
        ((ntraits + 1, mdev, draws_all), F32),
        ((nh, ntraits + 1, mdev, 128), F32),
        ((firms, 128), F32),
        ((rows, 128), F32),
        ((16, firms), BF16),
        ((firms, 128), BF16),
        ((nh, own, 128), F32),
        ((rows, 128), F32),
        ((ng, rows, 128), F32),
        ((1, 128), F32),
        ((ng, 1, 128), F32),
        ((mdev, 16, 128), BF16),
        ((mdev * 64, 256), BF16),
        ((256, 256), BF16),
        ((nh * mdev * 64, firms), BF16),
        ((nh, firms, mdev * 64), BF16),
        ((nh * mdev * 64, 128), F32),
        ((nh * mdev * 64, 128), F32),
        ((mdev * 64, 256), BF16),
        ((mdev * 64, 256), BF16),
        ((firms, 256), BF16),
        ((firms, 256), F32),
        ((ITERS, ng, rows, 128), F32),
        ((ITERS, ng - 1, rows, 128), F32),
        ((ITERS, nh, 8, 128), F32),
        ((ITERS, nh, 8, 128), F32),
        ((ITERS - 1, nh, 8, 128), F32),
        ((ITERS - 1, 8, 128), F32),
        ((ITERS - 1, rows, 128), F32),
        ((ITERS - 1, ng, rows, 128), F32),
        ((ITERS, 1, 128), F32),
        ((ITERS, ng, 1, 128), F32),
        ((ITERS, 1, 128), F32),
        ((ITERS, nh, 1, 128), F32),
        ((nh, own, 128), F32),
    ]
    stages = PER_STEP + 6 * ITERS
    return pl.pallas_call(
        functools.partial(kernel, dims),
        name="contraction",
        out_shape=(
            jax.ShapeDtypeStruct((mdev, 64), F32),
            jax.ShapeDtypeStruct((own, draws_all), F32),
        ),
        in_specs=[vmem, vmem, vmem, vmem, smem, smem, vmem, vmem, smem, vmem, anywhere, anywhere],
        out_specs=(vmem, vmem),
        scratch_shapes=[pltpu.VMEM(s, d) for s, d in scratch]
        + [
            pltpu.SemaphoreType.DMA((5,)),
            pltpu.SemaphoreType.DMA((stages,)),
            pltpu.SemaphoreType.DMA((stages,)),
            pltpu.SemaphoreType.DMA((nh,)),
            pltpu.SemaphoreType.DMA((nh,)),
        ],
        compiler_params=pltpu.CompilerParams(
            collective_id=0, has_side_effects=True, vmem_limit_bytes=60 * 1024 * 1024
        ),
    )(
        mean_utility,
        market_share,
        product_firm,
        product_traits.transpose(2, 0, 1),
        taste_scale,
        market_size,
        type_weight,
        loyalty,
        firm_order,
        firm_order.reshape(1, firms),
        taste_draws.transpose(1, 0, 2),
        firm_share,
    )


def solution(mesh):
    shape = (4, 4, 2, mesh.shape["grp"])
    torus = Mesh(mesh.devices.reshape(shape), AXES)
    in_specs = (
        P(AXES, None),
        P(AXES, None),
        P(AXES, None, None),
        P(AXES, None, None),
        P(),
        P(AXES, None),
        P(AXES),
        P(AXES, None),
        P(),
        P(AXES, None),
        P(),
    )
    out_specs = (P(AXES, None), P(AXES, None))
    return jax.shard_map(
        functools.partial(local, shape=shape),
        mesh=torus,
        in_specs=in_specs,
        out_specs=out_specs,
        check_vma=False,
    )
```

```python
import functools

import jax
import jax.numpy as jnp
from jax import lax
from jax.experimental import pallas as pl
from jax.experimental.pallas import tpu as pltpu
from jax.sharding import Mesh
from jax.sharding import PartitionSpec as P

ITERS = 3
CLIP_TARGET = 0.5
NORM_EPS = 1e-06
AXES = ("mkt_0", "mkt_1", "mkt_2", "grp")
MESH = pl.DeviceIdType.MESH
F32 = jnp.float32
BF16 = jnp.bfloat16
PK, SHOCK, LOY, TABLE, TMASS, OUT, PER_STEP = 0, 1, 2, 3, 4, 5, 6
PRED, RS, DMEAN, SQ_G, SQ_H, AG, STEP_STAGES = 0, 1, 2, 3, 4, 5, 6
LOG2E = 1.4426950408889634


def split_hi_lo(value):
    hi = value.astype(BF16)
    lo = (value - hi.astype(F32)).astype(BF16)
    return hi, lo


def kernel(
    dims,
    mean_ref,
    share_ref,
    firm_ref,
    traits_ref,
    scale_ref,
    size_ref,
    weight_ref,
    loy_ref,
    order_ref,
    order_row_ref,
    draws_hbm,
    fshare_hbm,
    mean_out,
    loy_out,
    square,
    pk_own,
    pk,
    shock_own,
    shock,
    fshare,
    fs_own,
    order_row_b,
    order_col_b,
    loy_in,
    own_table,
    table,
    tmass_s,
    tmass_r,
    lane_mask,
    traits_l,
    shocks_r,
    onehot,
    onehot_t,
    util,
    gsum,
    weighted_0,
    weighted_1,
    weighted_2,
    weighted_3,
    terms,
    acc,
    part,
    rs,
    pred,
    pred_r,
    dmean,
    dmean_s,
    gap_s,
    ag,
    sq_s,
    sq_r,
    sq2_s,
    sq2_r,
    fin_s,
    fin,
    loc_sem,
    send,
    recv,
    recv_pk,
    recv_shock,
):
    nx, nz, nc, ny, mdev, ntraits, firms, draws_all, own = dims
    weighted = (weighted_0, weighted_1, weighted_2, weighted_3)
    nh = nc * ny
    ng = nx * nz
    rows = firms // ng
    mrows = mdev * 64
    x, z, c, y = (lax.axis_index(a) for a in AXES)
    g = x * nz + z
    h = c * ny + y
    dys = (0, 1, 3, 2)
    hpeers = [(i % nc, dys[i // nc]) for i in range(1, nh)]
    far = {0: 0, 1: 1, 2: 2, 3: 1}
    gpeers = [(dx, dz) for dx in range(nx) for dz in range(nz) if (dx, dz) != (0, 0)]
    gpeers.sort(key=lambda d: -far[d[0]] - far[d[1]])

    def hdev(dc, dy):
        return lax.rem(c + dc, nc), lax.rem(y + dy, ny)

    def gdev(dx, dz):
        return lax.rem(x + dx, nx), lax.rem(z + dz, nz)

    def source(i):
        q = i // nc
        dy = q + q // 2 - 2 * (q // 3)
        return lax.rem(c + lax.rem(i, nc), nc) * ny + lax.rem(y + dy, ny)

    def lanes(index):
        return pl.ds(pl.multiple_of(index * 128, 128), 128)

    started = []

    def push(stage, src, dst, device, sem=None):
        pltpu.make_async_remote_copy(
            src_ref=src,
            dst_ref=dst,
            send_sem=send.at[stage],
            recv_sem=recv.at[stage] if sem is None else sem,
            device_id=device,
            device_id_type=MESH,
        ).start()

    def to_h(stage, src_of, dst, sems=None):
        for dc, dy in hpeers:
            c2, y2 = hdev(dc, dy)
            slot = dc + nc * dys.index((ny - dy) % ny)
            sem = None if sems is None else sems.at[slot]
            push(stage, src_of(c2 * ny + y2), dst, (x, z, c2, y2), sem)

    def to_g(stage, src_of, dst_of):
        for dx, dz in gpeers:
            x2, z2 = gdev(dx, dz)
            push(stage, src_of(x2 * nz + z2), dst_of(dx * nz + dz), (x2, z2, c, y))

    def arrived(stage, like):
        started.append((stage, like))
        pltpu.make_async_copy(like, like, recv.at[stage]).wait()

    def keep(src, dst, sem):
        copy = pltpu.make_async_copy(src, dst, sem)
        copy.start()
        return copy

    get_draws = keep(draws_hbm, shock_own.at[pl.ds(0, ntraits)], loc_sem.at[0])
    get_share = keep(fshare_hbm.at[:, lanes(h)], fshare, loc_sem.at[1])

    barrier = pltpu.get_barrier_semaphore()
    for dc, dy in hpeers:
        c2, y2 = hdev(dc, dy)
        pl.semaphore_signal(barrier, inc=1, device_id=(x, z, c2, y2), device_id_type=MESH)
    for dx, dz in gpeers:
        x2, z2 = gdev(dx, dz)
        pl.semaphore_signal(barrier, inc=1, device_id=(x2, z2, c, y), device_id_type=MESH)

    lane = lax.broadcasted_iota(jnp.int32, (8, 128), 1)
    lane_jb, lane_m = lane // mdev, lax.rem(lane, mdev)
    lane16 = lax.broadcasted_iota(jnp.int32, (mdev, 128), 1)
    market = lax.broadcasted_iota(jnp.int32, (mdev, 128), 0)

    square[...] = jnp.zeros(square.shape, F32)
    for k in range(ntraits):
        square[k * mdev : (k + 1) * mdev, 0:64] = traits_ref[k] * (scale_ref[k] * LOG2E)
    mean_2 = mean_ref[...] * LOG2E
    mean_a = mean_2.astype(BF16).astype(F32)
    ids = firm_ref[...].astype(F32) - 256.0
    square[5 * mdev : 6 * mdev, 0:64] = mean_a
    square[6 * mdev : 7 * mdev, 0:64] = ids
    square[7 * mdev : 8 * mdev, 0:64] = mean_2 - mean_a
    pk_own[0:64, :] = square[...].T[0:64, :]
    for p in range(mdev // 2):
        even = square[6 * mdev + 2 * p : 6 * mdev + 2 * p + 1, :]
        odd = square[6 * mdev + 2 * p + 1 : 6 * mdev + 2 * p + 2, :]
        pk_own[64 + p : 65 + p, :] = even + pltpu.roll(odd, 64, 1)

    row_mass = None
    for m in range(mdev):
        shock_own[ntraits, m : m + 1, :] = weight_ref[m : m + 1, :] * size_ref[m]
    row_mass = jnp.sum(shock_own[ntraits], axis=1, keepdims=True)
    denom = jnp.sum(
        jnp.where(lax.rem(lane16, mdev) == market, row_mass, 0.0), axis=0, keepdims=True
    )

    order_f = order_row_ref[...].astype(F32) - 256.0
    for b in range(firms // 128):
        row = order_f[:, b * 128 : (b + 1) * 128]
        order_row_b[b] = jnp.broadcast_to(row, (16, 128)).astype(BF16)
        order_col_b[b * 128 : (b + 1) * 128, :] = jnp.broadcast_to(row, (128, 128)).T.astype(BF16)
    lane_b = lax.rem(lax.broadcasted_iota(jnp.int32, (16, 128), 1), mdev)
    for m in range(mdev):
        lane_mask[m] = jnp.where(lane_b == m, 1.0, 0.0).astype(BF16)
    kind = lax.rem(lax.broadcasted_iota(jnp.int32, (256, 128), 0) // mdev, 8)
    is_mean = jnp.logical_or(kind == 5, kind == 7)
    shocks_r[0] = jnp.where(is_mean, 1.0, 0.0).astype(BF16)
    shocks_r[1] = jnp.zeros((256, 128), BF16)

    def joined(ref):
        return jnp.concatenate([ref[k] for k in range(ref.shape[0])], axis=1)

    def folded(both):
        return both[:, :128] + both[:, 128:]

    def build(i, carry):
        hh = source(i)
        pltpu.make_async_copy(pk.at[hh], pk.at[hh], recv_pk.at[i]).wait()
        base = pl.multiple_of(hh * mrows, mrows)
        one = jnp.ones((16, 128), BF16)
        zero = jnp.zeros((16, 128), BF16)
        for m in range(mdev):
            at = 6 * mdev + m
            for b in range(4):
                col = jnp.broadcast_to(pk[hh, b * 16 : b * 16 + 16, at : at + 1], (16, 128))
                col = col.astype(BF16)
                where = pl.ds(pl.multiple_of(base + m * 64 + b * 16, 16), 16)
                for t in range(firms // 128):
                    onehot[t, where, :] = jnp.where(col == order_row_b[t], one, zero)
        for p in range(mdev // 2):
            row = jnp.broadcast_to(pk[hh, 64 + p : 65 + p, :], (16, 128)).astype(BF16)
            for t in range(firms // 16):
                at = t * 16
                hot = jnp.where(order_col_b[at : at + 16, :] == row, one, zero)
                onehot_t[hh, p, at : at + 16, :] = hot
        return carry

    def tastes(i, carry):
        hh = source(i)
        pltpu.make_async_copy(shock.at[hh], shock.at[hh], recv_shock.at[i]).wait()
        hi, lo = split_hi_lo(shock[hh, 0:ntraits].reshape(ntraits * mdev, 128))
        for part_of in range(2):
            at = part_of * 128
            shocks_r[0, at : at + ntraits * mdev, :] = hi
            shocks_r[1, at : at + ntraits * mdev, :] = lo
        hi, lo = split_hi_lo(pk[hh, 0:64, :])
        for m in range(mdev):
            mask = lane_mask[m]
            for b in range(4):
                at = m * 64 + b * 16
                traits_l[0, at : at + 16, :] = hi[b * 16 : b * 16 + 16] * mask
                traits_l[1, at : at + 16, :] = lo[b * 16 : b * 16 + 16] * mask
        base = pl.multiple_of(hh * mrows, mrows)
        both = jnp.dot(joined(traits_l), joined(shocks_r), preferred_element_type=F32)
        util[pl.ds(base, mrows), :] = folded(both)
        return carry

    def set_terms(source):
        hi, lo = split_hi_lo(source[...].reshape(firms, 128) * LOG2E)
        terms[0] = hi
        terms[1] = lo

    def gather():
        chunk = nh * mrows // 2

        def block(q, carry):
            where = pl.ds(pl.multiple_of(q * chunk, chunk), chunk)
            hot = jnp.concatenate([onehot[t, where, :] for t in range(firms // 128)], axis=1)
            both = jnp.dot(hot, joined(terms), preferred_element_type=F32)
            gsum[where, :] = folded(both)
            return carry

        lax.fori_loop(0, 2, block, 0)

    keep(pk_own, pk.at[h], recv_pk.at[0])
    get_draws.wait()
    keep(shock_own.at[:, :, lanes(h)], shock.at[h], recv_shock.at[0])
    build(0, 0)

    pl.semaphore_wait(barrier, len(hpeers) + len(gpeers))

    to_h(LOY, lambda h2: loy_ref.at[:, lanes(h2)], loy_in.at[h])
    keep_loy = keep(loy_ref.at[:, lanes(h)], loy_in.at[h], loc_sem.at[2])
    to_h(PK, lambda h2: pk_own, pk.at[h], recv_pk)
    to_h(SHOCK, lambda h2: shock_own.at[:, :, lanes(h2)], shock.at[h], recv_shock)
    started.append((PK, pk.at[pl.ds(0, nh - 1)]))
    started.append((SHOCK, shock.at[pl.ds(0, nh - 1)]))

    square[0:mdev, 0:64] = share_ref[...]
    turned = square[...].T
    log_share = jnp.zeros((8, 128), F32)
    for jb in range(8):
        block = turned[jb * 8 : jb * 8 + 8, :]
        if jb:
            block = pltpu.roll(block, jb * mdev, 1)
        log_share = jnp.where(lane // mdev == jb, block, log_share)
    log_share = jnp.log(log_share)
    get_share.wait()
    for k in range(rows):
        fs_own[k : k + 1, :] = fshare[pl.ds(order_ref[g * rows + k], 1), :]
    fs_own[...] = jnp.log(fs_own[...])
    tastes(0, 0)
    build(1, 0)

    keep_loy.wait()
    arrived(LOY, loy_in.at[pl.ds(0, nh - 1)])
    for hh in range(nh):
        own_table[hh * own : (hh + 1) * own, :] = loy_in[hh]
    to_g(TABLE, lambda g2: own_table, lambda slot: table.at[g])
    keep_own = keep(own_table, table.at[g], loc_sem.at[3])

    lax.fori_loop(2, nh, build, 0)
    lax.fori_loop(1, nh, tastes, 0)
    keep_own.wait()
    arrived(TABLE, table.at[pl.ds(0, ng - 1)])
    set_terms(table)
    gather()
    tm = jnp.sum(shock[:, ntraits].reshape(nh * mdev, 128), axis=0, keepdims=True)
    tmass_s[...] = tm
    to_g(TMASS, lambda g2: tmass_s, lambda slot: tmass_r.at[slot])

    delta_sum = jnp.zeros((8, 128), F32)
    type_mass = None
    clip = None

    def clip_of(step):
        sq = jnp.sum(jnp.sum(sq2_r[step], axis=0), axis=1, keepdims=True)
        return jnp.minimum(1.0, CLIP_TARGET / jnp.sqrt(sq / (firms * draws_all) + NORM_EPS))

    own_new = own_table[...]

    for step in range(ITERS):
        stage = PER_STEP + STEP_STAGES * step

        if step:
            before = stage - STEP_STAGES
            arrived(before + SQ_H, sq2_r.at[step - 1, pl.ds(0, nh - 1)])
            clip = clip_of(step - 1)
            own_new = own_new + clip * gap

        def choices(hh, weighted, step=step, clip=clip):
            base = pl.multiple_of(hh * mrows, mrows)
            compact = jnp.zeros((8, 128), F32)
            for m in range(mdev):
                expu = []
                total = None
                for jb in range(8):
                    where = pl.ds(pl.multiple_of(base + m * 64 + jb * 8, 8), 8)
                    moved = gsum[where, :]
                    u = util[where, :] + (clip * moved if step else moved)
                    if step < ITERS - 1:
                        util[where, :] = u
                    e = jnp.exp2(u)
                    expu.append(e)
                    total = e if total is None else total + e
                total = jnp.sum(total, axis=0, keepdims=True)
                scale = shock[hh, ntraits, m : m + 1, :] / (1.0 + total)
                reds = None
                for jb in range(0, 8, 2):
                    at = m * 64 + jb * 8
                    wts = [expu[jb] * scale, expu[jb + 1] * scale]
                    for k in range(2):
                        red = jnp.sum(wts[k], axis=1, keepdims=True)
                        reds = red if reds is None else jnp.where(lane_jb == jb + k, red, reds)
                    hi, lo = split_hi_lo(jnp.concatenate(wts, axis=0))
                    weighted[0, at : at + 16, :] = hi
                    weighted[1, at : at + 16, :] = lo
                compact = jnp.where(lane_m == m, reds, compact)
            pred[step, hh] = compact

        def collected(hh, weighted):
            return jnp.dot(joined(onehot_t.at[hh]), joined(weighted), preferred_element_type=F32)

        def four_blocks(q, carry):
            sums = collected(jnp.maximum(4 * q - 1, 0), weighted[3])
            for k in range(4):
                choices(4 * q + k, weighted[k])
                if k < 3:
                    sums = sums + collected(4 * q + k, weighted[k])
            acc[...] = acc[...] + sums
            return carry

        acc[...] = jnp.zeros(acc.shape, F32)
        weighted[3][...] = jnp.zeros(weighted[3].shape, BF16)
        lax.fori_loop(0, nh // 4, four_blocks, 0)

        last = acc[...] + collected(nh - 1, weighted[3])
        part[step] = (last[:, :128] + last[:, 128:]).reshape(ng, rows, 128)
        to_g(stage + RS, lambda g2: part.at[step, g2], lambda slot: rs.at[step, slot - 1])
        to_h(stage + PRED, lambda h2: pred.at[step, h2], pred_r.at[step, h])

        arrived(stage + PRED, pred_r.at[step, pl.ds(0, nh - 1)])
        pred_r[step, h] = pred[step, h]
        num = jnp.sum(pred_r[step], axis=0)
        delta = log_share - jnp.log(num / denom)
        delta_sum = delta_sum + delta
        if step < ITERS - 1:
            dmean_s[step] = delta * LOG2E
            dmean[step, h] = delta * LOG2E
            to_h(stage + DMEAN, lambda h2: dmean_s.at[step], dmean.at[step, h])
        if step == 0:
            arrived(TMASS, tmass_r.at[pl.ds(1, ng - 1)])
            type_mass = tmass_s[...]
            for slot in range(1, ng):
                type_mass = type_mass + tmass_r[slot]

        arrived(stage + RS, rs.at[step])
        totals = part[step, g]
        for slot in range(ng - 1):
            totals = totals + rs[step, slot]
        gap = fs_own[...] - jnp.log(totals / type_mass)
        sq = jnp.sum(gap * gap, axis=0, keepdims=True)
        sq_s[step] = sq
        sq_r[step, 0] = sq
        to_g(stage + SQ_G, lambda g2: sq_s.at[step], lambda slot: sq_r.at[step, slot])
        if step < ITERS - 1:
            gap_s[step] = gap
            ag[step, g] = gap
            to_g(stage + AG, lambda g2: gap_s.at[step], lambda slot: ag.at[step, g])
            arrived(stage + DMEAN, dmean.at[step, pl.ds(0, nh - 1)])

            def shift(hh, carry, step=step):
                base = pl.multiple_of(hh * mrows, mrows)
                cols = dmean[step, hh]
                for m in range(mdev):
                    for jb in range(8):
                        where = pl.ds(pl.multiple_of(base + m * 64 + jb * 8, 8), 8)
                        at = jb * mdev + m
                        util[where, :] = util[where, :] + cols[:, at : at + 1]
                return carry

            lax.fori_loop(0, nh, shift, 0)
        else:
            for hh in range(nh):
                fin_s[hh, 0] = own_new[hh * own : (hh + 1) * own, :]
                fin_s[hh, 1] = gap[hh * own : (hh + 1) * own, :]
            to_h(OUT, lambda h2: fin_s.at[h2], fin.at[h])
            keep_out = keep(fin_s.at[h], fin.at[h], loc_sem.at[4])
            square[0:8, :] = delta_sum
            turned = square[...].T
            natural = jnp.zeros((mdev, 128), F32)
            for jb in range(8):
                block = turned[jb * mdev : (jb + 1) * mdev, :]
                if jb:
                    block = pltpu.roll(block, jb * 8, 1)
                natural = jnp.where(lane16 // 8 == jb, block, natural)
            mean_out[...] = mean_ref[...] + natural[:, 0:64]
        arrived(stage + SQ_G, sq_r.at[step, pl.ds(1, ng - 1)])
        sq = jnp.sum(sq_r[step], axis=0)
        sq2_s[step] = sq
        sq2_r[step, h] = sq
        to_h(stage + SQ_H, lambda h2: sq2_s.at[step], sq2_r.at[step, h])
        if step < ITERS - 1:
            arrived(stage + AG, ag.at[step, pl.ds(0, ng - 1)])
            set_terms(ag.at[step])
            gather()

    keep_out.wait()
    arrived(OUT, fin.at[pl.ds(0, nh - 1)])
    stage = PER_STEP + STEP_STAGES * (ITERS - 1)
    for at, like in started:
        pltpu.make_async_copy(like, like, send.at[at]).wait()
    arrived(stage + SQ_H, sq2_r.at[ITERS - 1, pl.ds(0, nh - 1)])
    clip = clip_of(ITERS - 1)
    for hh in range(nh):
        loy_out[:, hh * 128 : (hh + 1) * 128] = fin[hh, 0] + clip * fin[hh, 1]
    like = sq2_r.at[ITERS - 1, pl.ds(0, nh - 1)]
    pltpu.make_async_copy(like, like, send.at[stage + SQ_H]).wait()


def handed_on(mean_ref, loy_ref, mean_out, loy_out):
    mean_out[...] = mean_ref[...]
    loy_out[...] = loy_ref[...]


def local(
    mean_utility,
    market_share,
    product_traits,
    taste_draws,
    taste_scale,
    type_weight,
    market_size,
    product_firm,
    firm_order,
    loyalty,
    firm_share,
    shape,
):
    nx, nz, nc, ny = shape
    nh, ng = nc * ny, nx * nz
    mdev, ntraits, draws_all = taste_draws.shape
    firms = firm_share.shape[0]
    own = loyalty.shape[0]
    rows = firms // ng
    dims = (nx, nz, nc, ny, mdev, ntraits, firms, draws_all, own)
    vmem = pl.BlockSpec(memory_space=pltpu.VMEM)
    smem = pl.BlockSpec(memory_space=pltpu.SMEM)
    anywhere = pl.BlockSpec(memory_space=pl.ANY)
    scratch = [
        ((128, 128), F32),
        ((72, 128), F32),
        ((nh, 72, 128), F32),
        ((ntraits + 1, mdev, draws_all), F32),
        ((nh, ntraits + 1, mdev, 128), F32),
        ((firms, 128), F32),
        ((rows, 128), F32),
        ((firms // 128, 16, 128), BF16),
        ((firms, 128), BF16),
        ((nh, own, 128), F32),
        ((rows, 128), F32),
        ((ng, rows, 128), F32),
        ((1, 128), F32),
        ((ng, 1, 128), F32),
        ((mdev, 16, 128), BF16),
        ((2, mdev * 64, 128), BF16),
        ((2, 256, 128), BF16),
        ((firms // 128, nh * mdev * 64, 128), BF16),
        ((nh, mdev // 2, firms, 128), BF16),
        ((nh * mdev * 64, 128), F32),
        ((nh * mdev * 64, 128), F32),
        ((2, mdev * 64, 128), BF16),
        ((2, mdev * 64, 128), BF16),
        ((2, mdev * 64, 128), BF16),
        ((2, mdev * 64, 128), BF16),
        ((2, firms, 128), BF16),
        ((firms, 256), F32),
        ((ITERS, ng, rows, 128), F32),
        ((ITERS, ng - 1, rows, 128), F32),
        ((ITERS, nh, 8, 128), F32),
        ((ITERS, nh, 8, 128), F32),
        ((ITERS - 1, nh, 8, 128), F32),
        ((ITERS - 1, 8, 128), F32),
        ((ITERS - 1, rows, 128), F32),
        ((ITERS - 1, ng, rows, 128), F32),
        ((ITERS, 1, 128), F32),
        ((ITERS, ng, 1, 128), F32),
        ((ITERS, 1, 128), F32),
        ((ITERS, nh, 1, 128), F32),
        ((nh, 2, own, 128), F32),
        ((nh, 2, own, 128), F32),
    ]
    stages = PER_STEP + STEP_STAGES * ITERS
    results = pl.pallas_call(
        functools.partial(kernel, dims),
        name="contraction",
        out_shape=(
            jax.ShapeDtypeStruct((mdev, 64), F32),
            jax.ShapeDtypeStruct((own, draws_all), F32),
        ),
        in_specs=[vmem, vmem, vmem, vmem, smem, smem, vmem, vmem, smem, vmem, anywhere, anywhere],
        out_specs=(vmem, vmem),
        scratch_shapes=[pltpu.VMEM(s, d) for s, d in scratch]
        + [
            pltpu.SemaphoreType.DMA((5,)),
            pltpu.SemaphoreType.DMA((stages,)),
            pltpu.SemaphoreType.DMA((stages,)),
            pltpu.SemaphoreType.DMA((nh,)),
            pltpu.SemaphoreType.DMA((nh,)),
        ],
        compiler_params=pltpu.CompilerParams(
            collective_id=0, has_side_effects=True, vmem_limit_bytes=60 * 1024 * 1024
        ),
    )(
        mean_utility,
        market_share,
        product_firm,
        product_traits.transpose(2, 0, 1),
        taste_scale,
        market_size,
        type_weight,
        loyalty,
        firm_order,
        firm_order.reshape(1, firms),
        taste_draws.transpose(1, 0, 2),
        firm_share,
    )
    return pl.pallas_call(
        handed_on,
        name="handed_on",
        out_shape=tuple(jax.ShapeDtypeStruct(r.shape, F32) for r in results),
        in_specs=[vmem, vmem],
        out_specs=(vmem, vmem),
    )(*results)


def solution(mesh):
    shape = (4, 4, 2, mesh.shape["grp"])
    torus = Mesh(mesh.devices.reshape(shape), AXES)
    in_specs = (
        P(AXES, None),
        P(AXES, None),
        P(AXES, None, None),
        P(AXES, None, None),
        P(),
        P(AXES, None),
        P(AXES),
        P(AXES, None),
        P(),
        P(AXES, None),
        P(),
    )
    out_specs = (P(AXES, None), P(AXES, None))
    return jax.shard_map(
        functools.partial(local, shape=shape),
        mesh=torus,
        in_specs=in_specs,
        out_specs=out_specs,
        check_vma=False,
    )
```

```python
import functools

import jax
import jax.numpy as jnp
from jax import lax
from jax.experimental import pallas as pl
from jax.experimental.pallas import tpu as pltpu
from jax.sharding import Mesh
from jax.sharding import PartitionSpec as P

ITERS = 3
CLIP_TARGET = 0.5
NORM_EPS = 1e-06
AXES = ("mkt_0", "mkt_1", "mkt_2", "grp")
MESH = pl.DeviceIdType.MESH
F32 = jnp.float32
BF16 = jnp.bfloat16
PK, SHOCK, LOY, TABLE, TMASS, OUT, PER_STEP = 0, 1, 2, 3, 4, 5, 6
PRED, RS, DMEAN, SQ_G, SQ_H, AG, STEP_STAGES = 0, 1, 2, 3, 4, 5, 6
LOG2E = 1.4426950408889634


def split_hi_lo(value):
    hi = value.astype(BF16)
    lo = (value - hi.astype(F32)).astype(BF16)
    return hi, lo


def kernel(
    dims,
    mean_hbm,
    share_hbm,
    firm_hbm,
    traits_hbm,
    scale_hbm,
    size_hbm,
    weight_hbm,
    loy_hbm,
    order_hbm,
    order_row_hbm,
    draws_hbm,
    fshare_hbm,
    mean_out,
    loy_out,
    mean_ref,
    share_ref,
    firm_ref,
    traits_ref,
    weight_ref,
    loy_ref,
    order_row_ref,
    scale_ref,
    size_ref,
    order_ref,
    square,
    pk_own,
    pk,
    shock_own,
    shock,
    fshare,
    fs_own,
    order_row_b,
    order_col_b,
    loy_in,
    own_table,
    table,
    tmass_s,
    tmass_r,
    lane_mask,
    traits_l,
    shocks_r,
    onehot,
    onehot_t,
    util,
    gsum,
    weighted_0,
    weighted_1,
    weighted_2,
    weighted_3,
    terms,
    acc,
    part,
    rs,
    pred,
    pred_r,
    dmean,
    dmean_s,
    gap_s,
    ag,
    sq_s,
    sq_r,
    sq2_s,
    sq2_r,
    fin_s,
    fin,
    loc_sem,
    send,
    recv,
    recv_pk,
    recv_shock,
):
    nx, nz, nc, ny, mdev, ntraits, firms, draws_all, own = dims
    weighted = (weighted_0, weighted_1, weighted_2, weighted_3)
    nh = nc * ny
    ng = nx * nz
    rows = firms // ng
    mrows = mdev * 64
    x, z, c, y = (lax.axis_index(a) for a in AXES)
    g = x * nz + z
    h = c * ny + y
    dys = (0, 1, 3, 2)
    hpeers = [(i % nc, dys[i // nc]) for i in range(1, nh)]
    far = {0: 0, 1: 1, 2: 2, 3: 1}
    gpeers = [(dx, dz) for dx in range(nx) for dz in range(nz) if (dx, dz) != (0, 0)]
    gpeers.sort(key=lambda d: -far[d[0]] - far[d[1]])

    def hdev(dc, dy):
        return lax.rem(c + dc, nc), lax.rem(y + dy, ny)

    def gdev(dx, dz):
        return lax.rem(x + dx, nx), lax.rem(z + dz, nz)

    def source(i):
        q = i // nc
        dy = q + q // 2 - 2 * (q // 3)
        return lax.rem(c + lax.rem(i, nc), nc) * ny + lax.rem(y + dy, ny)

    def lanes(index):
        return pl.ds(pl.multiple_of(index * 128, 128), 128)

    started = []

    def push(stage, src, dst, device, sem=None):
        pltpu.make_async_remote_copy(
            src_ref=src,
            dst_ref=dst,
            send_sem=send.at[stage],
            recv_sem=recv.at[stage] if sem is None else sem,
            device_id=device,
            device_id_type=MESH,
        ).start()

    def to_h(stage, src_of, dst, sems=None):
        for dc, dy in hpeers:
            c2, y2 = hdev(dc, dy)
            slot = dc + nc * dys.index((ny - dy) % ny)
            sem = None if sems is None else sems.at[slot]
            push(stage, src_of(c2 * ny + y2), dst, (x, z, c2, y2), sem)

    def to_g(stage, src_of, dst_of):
        for dx, dz in gpeers:
            x2, z2 = gdev(dx, dz)
            push(stage, src_of(x2 * nz + z2), dst_of(dx * nz + dz), (x2, z2, c, y))

    def arrived(stage, like):
        started.append((stage, like))
        pltpu.make_async_copy(like, like, recv.at[stage]).wait()

    def keep(src, dst, sem):
        copy = pltpu.make_async_copy(src, dst, sem)
        copy.start()
        return copy

    barrier = pltpu.get_barrier_semaphore()
    for dc, dy in hpeers:
        c2, y2 = hdev(dc, dy)
        pl.semaphore_signal(barrier, inc=1, device_id=(x, z, c2, y2), device_id_type=MESH)
    for dx, dz in gpeers:
        x2, z2 = gdev(dx, dz)
        pl.semaphore_signal(barrier, inc=1, device_id=(x2, z2, c, y), device_id_type=MESH)

    fetched = [
        keep(src, dst, loc_sem.at[5 + k])
        for k, (src, dst) in enumerate(
            [
                (traits_hbm, traits_ref),
                (mean_hbm, mean_ref),
                (firm_hbm, firm_ref),
                (order_row_hbm, order_row_ref),
                (weight_hbm, weight_ref),
                (loy_hbm, loy_ref),
                (share_hbm, share_ref),
                (scale_hbm, scale_ref),
                (size_hbm, size_ref),
                (order_hbm, order_ref),
            ]
        )
    ]
    get_draws = keep(draws_hbm, shock_own.at[pl.ds(0, ntraits)], loc_sem.at[0])
    get_share = keep(fshare_hbm.at[:, lanes(h)], fshare, loc_sem.at[1])

    lane = lax.broadcasted_iota(jnp.int32, (8, 128), 1)
    lane_jb, lane_m = lane // mdev, lax.rem(lane, mdev)
    lane16 = lax.broadcasted_iota(jnp.int32, (mdev, 128), 1)
    market = lax.broadcasted_iota(jnp.int32, (mdev, 128), 0)

    for copy in fetched:
        copy.wait()
    square[...] = jnp.zeros(square.shape, F32)
    for k in range(ntraits):
        square[k * mdev : (k + 1) * mdev, 0:64] = traits_ref[k] * (scale_ref[k] * LOG2E)
    mean_2 = mean_ref[...] * LOG2E
    mean_a = mean_2.astype(BF16).astype(F32)
    ids = firm_ref[...].astype(F32) - 256.0
    square[5 * mdev : 6 * mdev, 0:64] = mean_a
    square[6 * mdev : 7 * mdev, 0:64] = ids
    square[7 * mdev : 8 * mdev, 0:64] = mean_2 - mean_a
    pk_own[0:64, :] = square[...].T[0:64, :]
    for p in range(mdev // 2):
        even = square[6 * mdev + 2 * p : 6 * mdev + 2 * p + 1, :]
        odd = square[6 * mdev + 2 * p + 1 : 6 * mdev + 2 * p + 2, :]
        pk_own[64 + p : 65 + p, :] = even + pltpu.roll(odd, 64, 1)

    row_mass = None
    for m in range(mdev):
        shock_own[ntraits, m : m + 1, :] = weight_ref[m : m + 1, :] * size_ref[m]
    row_mass = jnp.sum(shock_own[ntraits], axis=1, keepdims=True)
    denom = jnp.sum(
        jnp.where(lax.rem(lane16, mdev) == market, row_mass, 0.0), axis=0, keepdims=True
    )

    order_f = order_row_ref[...].astype(F32) - 256.0
    for b in range(firms // 128):
        row = order_f[:, b * 128 : (b + 1) * 128]
        order_row_b[b] = jnp.broadcast_to(row, (16, 128)).astype(BF16)
        order_col_b[b * 128 : (b + 1) * 128, :] = jnp.broadcast_to(row, (128, 128)).T.astype(BF16)
    lane_b = lax.rem(lax.broadcasted_iota(jnp.int32, (16, 128), 1), mdev)
    for m in range(mdev):
        lane_mask[m] = jnp.where(lane_b == m, 1.0, 0.0).astype(BF16)
    kind = lax.rem(lax.broadcasted_iota(jnp.int32, (256, 128), 0) // mdev, 8)
    is_mean = jnp.logical_or(kind == 5, kind == 7)
    shocks_r[0] = jnp.where(is_mean, 1.0, 0.0).astype(BF16)
    shocks_r[1] = jnp.zeros((256, 128), BF16)

    def joined(ref):
        return jnp.concatenate([ref[k] for k in range(ref.shape[0])], axis=1)

    def folded(both):
        return both[:, :128] + both[:, 128:]

    def build(i, carry):
        hh = source(i)
        pltpu.make_async_copy(pk.at[hh], pk.at[hh], recv_pk.at[i]).wait()
        base = pl.multiple_of(hh * mrows, mrows)
        one = jnp.ones((16, 128), BF16)
        zero = jnp.zeros((16, 128), BF16)
        for m in range(mdev):
            at = 6 * mdev + m
            for b in range(4):
                col = jnp.broadcast_to(pk[hh, b * 16 : b * 16 + 16, at : at + 1], (16, 128))
                col = col.astype(BF16)
                where = pl.ds(pl.multiple_of(base + m * 64 + b * 16, 16), 16)
                for t in range(firms // 128):
                    onehot[t, where, :] = jnp.where(col == order_row_b[t], one, zero)
        for p in range(mdev // 2):
            row = jnp.broadcast_to(pk[hh, 64 + p : 65 + p, :], (16, 128)).astype(BF16)
            for t in range(firms // 16):
                at = t * 16
                hot = jnp.where(order_col_b[at : at + 16, :] == row, one, zero)
                onehot_t[hh, p, at : at + 16, :] = hot
        return carry

    def tastes(i, carry):
        hh = source(i)
        pltpu.make_async_copy(shock.at[hh], shock.at[hh], recv_shock.at[i]).wait()
        hi, lo = split_hi_lo(shock[hh, 0:ntraits].reshape(ntraits * mdev, 128))
        for part_of in range(2):
            at = part_of * 128
            shocks_r[0, at : at + ntraits * mdev, :] = hi
            shocks_r[1, at : at + ntraits * mdev, :] = lo
        hi, lo = split_hi_lo(pk[hh, 0:64, :])
        for m in range(mdev):
            mask = lane_mask[m]
            for b in range(4):
                at = m * 64 + b * 16
                traits_l[0, at : at + 16, :] = hi[b * 16 : b * 16 + 16] * mask
                traits_l[1, at : at + 16, :] = lo[b * 16 : b * 16 + 16] * mask
        base = pl.multiple_of(hh * mrows, mrows)
        both = jnp.dot(joined(traits_l), joined(shocks_r), preferred_element_type=F32)
        util[pl.ds(base, mrows), :] = folded(both)
        return carry

    def set_terms(source):
        hi, lo = split_hi_lo(source[...].reshape(firms, 128) * LOG2E)
        terms[0] = hi
        terms[1] = lo

    def gather():
        chunk = nh * mrows // 2

        def block(q, carry):
            where = pl.ds(pl.multiple_of(q * chunk, chunk), chunk)
            hot = jnp.concatenate([onehot[t, where, :] for t in range(firms // 128)], axis=1)
            both = jnp.dot(hot, joined(terms), preferred_element_type=F32)
            gsum[where, :] = folded(both)
            return carry

        lax.fori_loop(0, 2, block, 0)

    keep(pk_own, pk.at[h], recv_pk.at[0])
    get_draws.wait()
    keep(shock_own.at[:, :, lanes(h)], shock.at[h], recv_shock.at[0])
    build(0, 0)

    pl.semaphore_wait(barrier, len(hpeers) + len(gpeers))

    to_h(LOY, lambda h2: loy_ref.at[:, lanes(h2)], loy_in.at[h])
    keep_loy = keep(loy_ref.at[:, lanes(h)], loy_in.at[h], loc_sem.at[2])
    to_h(PK, lambda h2: pk_own, pk.at[h], recv_pk)
    to_h(SHOCK, lambda h2: shock_own.at[:, :, lanes(h2)], shock.at[h], recv_shock)
    started.append((PK, pk.at[pl.ds(0, nh - 1)]))
    started.append((SHOCK, shock.at[pl.ds(0, nh - 1)]))

    square[0:mdev, 0:64] = share_ref[...]
    turned = square[...].T
    log_share = jnp.zeros((8, 128), F32)
    for jb in range(8):
        block = turned[jb * 8 : jb * 8 + 8, :]
        if jb:
            block = pltpu.roll(block, jb * mdev, 1)
        log_share = jnp.where(lane // mdev == jb, block, log_share)
    log_share = jnp.log(log_share)
    get_share.wait()
    for k in range(rows):
        fs_own[k : k + 1, :] = fshare[pl.ds(order_ref[g * rows + k], 1), :]
    fs_own[...] = jnp.log(fs_own[...])
    tastes(0, 0)
    build(1, 0)

    keep_loy.wait()
    arrived(LOY, loy_in.at[pl.ds(0, nh - 1)])
    for hh in range(nh):
        own_table[hh * own : (hh + 1) * own, :] = loy_in[hh]
    to_g(TABLE, lambda g2: own_table, lambda slot: table.at[g])
    keep_own = keep(own_table, table.at[g], loc_sem.at[3])

    lax.fori_loop(2, nh, build, 0)
    lax.fori_loop(1, nh, tastes, 0)
    keep_own.wait()
    arrived(TABLE, table.at[pl.ds(0, ng - 1)])
    set_terms(table)
    gather()
    tm = jnp.sum(shock[:, ntraits].reshape(nh * mdev, 128), axis=0, keepdims=True)
    tmass_s[...] = tm
    to_g(TMASS, lambda g2: tmass_s, lambda slot: tmass_r.at[slot])

    delta_sum = jnp.zeros((8, 128), F32)
    type_mass = None
    clip = None

    def clip_of(step):
        sq = jnp.sum(jnp.sum(sq2_r[step], axis=0), axis=1, keepdims=True)
        return jnp.minimum(1.0, CLIP_TARGET / jnp.sqrt(sq / (firms * draws_all) + NORM_EPS))

    own_new = own_table[...]

    for step in range(ITERS):
        stage = PER_STEP + STEP_STAGES * step

        if step:
            before = stage - STEP_STAGES
            arrived(before + SQ_H, sq2_r.at[step - 1, pl.ds(0, nh - 1)])
            clip = clip_of(step - 1)
            own_new = own_new + clip * gap

        def choices(hh, weighted, step=step, clip=clip):
            base = pl.multiple_of(hh * mrows, mrows)
            compact = jnp.zeros((8, 128), F32)
            for m in range(mdev):
                expu = []
                total = None
                for jb in range(8):
                    where = pl.ds(pl.multiple_of(base + m * 64 + jb * 8, 8), 8)
                    moved = gsum[where, :]
                    u = util[where, :] + (clip * moved if step else moved)
                    if step < ITERS - 1:
                        util[where, :] = u
                    e = jnp.exp2(u)
                    expu.append(e)
                    total = e if total is None else total + e
                total = jnp.sum(total, axis=0, keepdims=True)
                scale = shock[hh, ntraits, m : m + 1, :] / (1.0 + total)
                reds = None
                for jb in range(0, 8, 2):
                    at = m * 64 + jb * 8
                    wts = [expu[jb] * scale, expu[jb + 1] * scale]
                    for k in range(2):
                        red = jnp.sum(wts[k], axis=1, keepdims=True)
                        reds = red if reds is None else jnp.where(lane_jb == jb + k, red, reds)
                    hi, lo = split_hi_lo(jnp.concatenate(wts, axis=0))
                    weighted[0, at : at + 16, :] = hi
                    weighted[1, at : at + 16, :] = lo
                compact = jnp.where(lane_m == m, reds, compact)
            pred[step, hh] = compact

        def collected(hh, weighted):
            return jnp.dot(joined(onehot_t.at[hh]), joined(weighted), preferred_element_type=F32)

        def four_blocks(q, carry):
            sums = collected(jnp.maximum(4 * q - 1, 0), weighted[3])
            for k in range(4):
                choices(4 * q + k, weighted[k])
                if k < 3:
                    sums = sums + collected(4 * q + k, weighted[k])
            acc[...] = acc[...] + sums
            return carry

        acc[...] = jnp.zeros(acc.shape, F32)
        weighted[3][...] = jnp.zeros(weighted[3].shape, BF16)
        lax.fori_loop(0, nh // 4, four_blocks, 0)

        last = acc[...] + collected(nh - 1, weighted[3])
        part[step] = (last[:, :128] + last[:, 128:]).reshape(ng, rows, 128)
        to_g(stage + RS, lambda g2: part.at[step, g2], lambda slot: rs.at[step, slot - 1])
        to_h(stage + PRED, lambda h2: pred.at[step, h2], pred_r.at[step, h])

        arrived(stage + PRED, pred_r.at[step, pl.ds(0, nh - 1)])
        pred_r[step, h] = pred[step, h]
        num = jnp.sum(pred_r[step], axis=0)
        delta = log_share - jnp.log(num / denom)
        delta_sum = delta_sum + delta
        if step < ITERS - 1:
            dmean_s[step] = delta * LOG2E
            dmean[step, h] = delta * LOG2E
            to_h(stage + DMEAN, lambda h2: dmean_s.at[step], dmean.at[step, h])
        if step == 0:
            arrived(TMASS, tmass_r.at[pl.ds(1, ng - 1)])
            type_mass = tmass_s[...]
            for slot in range(1, ng):
                type_mass = type_mass + tmass_r[slot]

        arrived(stage + RS, rs.at[step])
        totals = part[step, g]
        for slot in range(ng - 1):
            totals = totals + rs[step, slot]
        gap = fs_own[...] - jnp.log(totals / type_mass)
        sq = jnp.sum(gap * gap, axis=0, keepdims=True)
        sq_s[step] = sq
        sq_r[step, 0] = sq
        to_g(stage + SQ_G, lambda g2: sq_s.at[step], lambda slot: sq_r.at[step, slot])
        if step < ITERS - 1:
            gap_s[step] = gap
            ag[step, g] = gap
            to_g(stage + AG, lambda g2: gap_s.at[step], lambda slot: ag.at[step, g])
            arrived(stage + DMEAN, dmean.at[step, pl.ds(0, nh - 1)])

            def shift(hh, carry, step=step):
                base = pl.multiple_of(hh * mrows, mrows)
                cols = dmean[step, hh]
                for m in range(mdev):
                    for jb in range(8):
                        where = pl.ds(pl.multiple_of(base + m * 64 + jb * 8, 8), 8)
                        at = jb * mdev + m
                        util[where, :] = util[where, :] + cols[:, at : at + 1]
                return carry

            lax.fori_loop(0, nh, shift, 0)
        else:
            for hh in range(nh):
                fin_s[hh, 0] = own_new[hh * own : (hh + 1) * own, :]
                fin_s[hh, 1] = gap[hh * own : (hh + 1) * own, :]
            to_h(OUT, lambda h2: fin_s.at[h2], fin.at[h])
            keep_out = keep(fin_s.at[h], fin.at[h], loc_sem.at[4])
            square[0:8, :] = delta_sum
            turned = square[...].T
            natural = jnp.zeros((mdev, 128), F32)
            for jb in range(8):
                block = turned[jb * mdev : (jb + 1) * mdev, :]
                if jb:
                    block = pltpu.roll(block, jb * 8, 1)
                natural = jnp.where(lane16 // 8 == jb, block, natural)
            mean_out[...] = mean_ref[...] + natural[:, 0:64]
        arrived(stage + SQ_G, sq_r.at[step, pl.ds(1, ng - 1)])
        sq = jnp.sum(sq_r[step], axis=0)
        sq2_s[step] = sq
        sq2_r[step, h] = sq
        to_h(stage + SQ_H, lambda h2: sq2_s.at[step], sq2_r.at[step, h])
        if step < ITERS - 1:
            arrived(stage + AG, ag.at[step, pl.ds(0, ng - 1)])
            set_terms(ag.at[step])
            gather()

    keep_out.wait()
    arrived(OUT, fin.at[pl.ds(0, nh - 1)])
    stage = PER_STEP + STEP_STAGES * (ITERS - 1)
    for at, like in started:
        pltpu.make_async_copy(like, like, send.at[at]).wait()
    arrived(stage + SQ_H, sq2_r.at[ITERS - 1, pl.ds(0, nh - 1)])
    clip = clip_of(ITERS - 1)
    for hh in range(nh):
        loy_out[:, hh * 128 : (hh + 1) * 128] = fin[hh, 0] + clip * fin[hh, 1]
    like = sq2_r.at[ITERS - 1, pl.ds(0, nh - 1)]
    pltpu.make_async_copy(like, like, send.at[stage + SQ_H]).wait()


def handed_on(mean_ref, loy_ref, mean_out, loy_out):
    mean_out[...] = mean_ref[...]
    loy_out[...] = loy_ref[...]


def local(
    mean_utility,
    market_share,
    product_traits,
    taste_draws,
    taste_scale,
    type_weight,
    market_size,
    product_firm,
    firm_order,
    loyalty,
    firm_share,
    shape,
):
    nx, nz, nc, ny = shape
    nh, ng = nc * ny, nx * nz
    mdev, ntraits, draws_all = taste_draws.shape
    firms = firm_share.shape[0]
    own = loyalty.shape[0]
    rows = firms // ng
    dims = (nx, nz, nc, ny, mdev, ntraits, firms, draws_all, own)
    vmem = pl.BlockSpec(memory_space=pltpu.VMEM)
    anywhere = pl.BlockSpec(memory_space=pl.ANY)
    scratch = [
        ((mdev, 64), F32),
        ((mdev, 64), F32),
        ((mdev, 64), jnp.int32),
        ((ntraits, mdev, 64), F32),
        ((mdev, draws_all), F32),
        ((own, draws_all), F32),
        ((1, firms), jnp.int32),
        ((128, 128), F32),
        ((72, 128), F32),
        ((nh, 72, 128), F32),
        ((ntraits + 1, mdev, draws_all), F32),
        ((nh, ntraits + 1, mdev, 128), F32),
        ((firms, 128), F32),
        ((rows, 128), F32),
        ((firms // 128, 16, 128), BF16),
        ((firms, 128), BF16),
        ((nh, own, 128), F32),
        ((rows, 128), F32),
        ((ng, rows, 128), F32),
        ((1, 128), F32),
        ((ng, 1, 128), F32),
        ((mdev, 16, 128), BF16),
        ((2, mdev * 64, 128), BF16),
        ((2, 256, 128), BF16),
        ((firms // 128, nh * mdev * 64, 128), BF16),
        ((nh, mdev // 2, firms, 128), BF16),
        ((nh * mdev * 64, 128), F32),
        ((nh * mdev * 64, 128), F32),
        ((2, mdev * 64, 128), BF16),
        ((2, mdev * 64, 128), BF16),
        ((2, mdev * 64, 128), BF16),
        ((2, mdev * 64, 128), BF16),
        ((2, firms, 128), BF16),
        ((firms, 256), F32),
        ((ITERS, ng, rows, 128), F32),
        ((ITERS, ng - 1, rows, 128), F32),
        ((ITERS, nh, 8, 128), F32),
        ((ITERS, nh, 8, 128), F32),
        ((ITERS - 1, nh, 8, 128), F32),
        ((ITERS - 1, 8, 128), F32),
        ((ITERS - 1, rows, 128), F32),
        ((ITERS - 1, ng, rows, 128), F32),
        ((ITERS, 1, 128), F32),
        ((ITERS, ng, 1, 128), F32),
        ((ITERS, 1, 128), F32),
        ((ITERS, nh, 1, 128), F32),
        ((nh, 2, own, 128), F32),
        ((nh, 2, own, 128), F32),
    ]
    stages = PER_STEP + STEP_STAGES * ITERS
    results = pl.pallas_call(
        functools.partial(kernel, dims),
        name="contraction",
        out_shape=(
            jax.ShapeDtypeStruct((mdev, 64), F32),
            jax.ShapeDtypeStruct((own, draws_all), F32),
        ),
        in_specs=[anywhere] * 12,
        out_specs=(vmem, vmem),
        scratch_shapes=[pltpu.VMEM(s, d) for s, d in scratch[:7]]
        + [
            pltpu.SMEM((ntraits,), F32),
            pltpu.SMEM((mdev,), F32),
            pltpu.SMEM((firms,), jnp.int32),
        ]
        + [pltpu.VMEM(s, d) for s, d in scratch[7:]]
        + [
            pltpu.SemaphoreType.DMA((15,)),
            pltpu.SemaphoreType.DMA((stages,)),
            pltpu.SemaphoreType.DMA((stages,)),
            pltpu.SemaphoreType.DMA((nh,)),
            pltpu.SemaphoreType.DMA((nh,)),
        ],
        compiler_params=pltpu.CompilerParams(
            collective_id=0, has_side_effects=True, vmem_limit_bytes=60 * 1024 * 1024
        ),
    )(
        mean_utility,
        market_share,
        product_firm,
        product_traits.transpose(2, 0, 1),
        taste_scale,
        market_size,
        type_weight,
        loyalty,
        firm_order,
        firm_order.reshape(1, firms),
        taste_draws.transpose(1, 0, 2),
        firm_share,
    )
    return pl.pallas_call(
        handed_on,
        name="handed_on",
        out_shape=tuple(jax.ShapeDtypeStruct(r.shape, F32) for r in results),
        in_specs=[vmem, vmem],
        out_specs=(vmem, vmem),
    )(*results)


def solution(mesh):
    shape = (4, 4, 2, mesh.shape["grp"])
    torus = Mesh(mesh.devices.reshape(shape), AXES)
    in_specs = (
        P(AXES, None),
        P(AXES, None),
        P(AXES, None, None),
        P(AXES, None, None),
        P(),
        P(AXES, None),
        P(AXES),
        P(AXES, None),
        P(),
        P(AXES, None),
        P(),
    )
    out_specs = (P(AXES, None), P(AXES, None))
    return jax.shard_map(
        functools.partial(local, shape=shape),
        mesh=torus,
        in_specs=in_specs,
        out_specs=out_specs,
        check_vma=False,
    )
```

```python
import functools

import jax
import jax.numpy as jnp
from jax import lax
from jax.experimental import pallas as pl
from jax.experimental.pallas import tpu as pltpu
from jax.sharding import Mesh
from jax.sharding import PartitionSpec as P

ITERS = 3
CLIP_TARGET = 0.5
NORM_EPS = 1e-06
AXES = ("mkt_0", "mkt_1", "mkt_2", "grp")
MESH = pl.DeviceIdType.MESH
F32 = jnp.float32
BF16 = jnp.bfloat16
PK, SHOCK, LOY, TABLE, TMASS, OUT, PER_STEP = 0, 1, 2, 3, 4, 5, 6
PRED, RS, DMEAN, SQ_G, SQ_H, AG, STEP_STAGES = 0, 1, 2, 3, 4, 5, 6
LOG2E = 1.4426950408889634


def split_hi_lo(value):
    hi = value.astype(BF16)
    lo = (value - hi.astype(F32)).astype(BF16)
    return hi, lo


def kernel(
    dims,
    mean_hbm,
    share_hbm,
    firm_hbm,
    traits_hbm,
    scale_hbm,
    size_hbm,
    weight_hbm,
    loy_hbm,
    order_hbm,
    order_row_hbm,
    draws_hbm,
    fshare_hbm,
    mean_out,
    loy_out,
    mean_ref,
    share_ref,
    firm_ref,
    traits_ref,
    weight_ref,
    loy_ref,
    order_row_ref,
    scale_ref,
    size_ref,
    order_ref,
    square,
    pk_own,
    pk,
    shock_own,
    shock,
    fshare,
    fs_own,
    order_row_b,
    order_col_b,
    loy_in,
    own_table,
    table,
    tmass_s,
    tmass_r,
    lane_mask,
    traits_l,
    shocks_r,
    onehot,
    onehot_t,
    util,
    gsum,
    weighted_0,
    weighted_1,
    weighted_2,
    weighted_3,
    terms,
    acc,
    part,
    rs,
    pred,
    pred_r,
    dmean,
    dmean_s,
    gap_s,
    ag,
    sq_s,
    sq_r,
    sq2_s,
    sq2_r,
    fin_s,
    fin,
    loc_sem,
    send,
    recv,
    recv_pk,
    recv_shock,
):
    nx, nz, nc, ny, mdev, ntraits, firms, draws_all, own = dims
    weighted = (weighted_0, weighted_1, weighted_2, weighted_3)
    nh = nc * ny
    ng = nx * nz
    rows = firms // ng
    mrows = mdev * 64
    x, z, c, y = (lax.axis_index(a) for a in AXES)
    g = x * nz + z
    h = c * ny + y
    dys = (0, 1, 3, 2)
    hpeers = [(i % nc, dys[i // nc]) for i in range(1, nh)]
    far = {0: 0, 1: 1, 2: 2, 3: 1}
    gpeers = [(dx, dz) for dx in range(nx) for dz in range(nz) if (dx, dz) != (0, 0)]
    gpeers.sort(key=lambda d: -far[d[0]] - far[d[1]])

    def hdev(dc, dy):
        return lax.rem(c + dc, nc), lax.rem(y + dy, ny)

    def gdev(dx, dz):
        return lax.rem(x + dx, nx), lax.rem(z + dz, nz)

    def source(i):
        q = i // nc
        dy = q + q // 2 - 2 * (q // 3)
        return lax.rem(c + lax.rem(i, nc), nc) * ny + lax.rem(y + dy, ny)

    def lanes(index):
        return pl.ds(pl.multiple_of(index * 128, 128), 128)

    started = []

    def push(stage, src, dst, device, sem=None):
        pltpu.make_async_remote_copy(
            src_ref=src,
            dst_ref=dst,
            send_sem=send.at[stage],
            recv_sem=recv.at[stage] if sem is None else sem,
            device_id=device,
            device_id_type=MESH,
        ).start()

    def to_h(stage, src_of, dst, sems=None, only=None):
        for dc, dy in hpeers:
            if only is not None and not only(dc, dy):
                continue
            c2, y2 = hdev(dc, dy)
            slot = dc + nc * dys.index((ny - dy) % ny)
            sem = None if sems is None else sems.at[slot]
            push(stage, src_of(c2 * ny + y2), dst, (x, z, c2, y2), sem)

    def to_g(stage, src_of, dst_of):
        for dx, dz in gpeers:
            x2, z2 = gdev(dx, dz)
            push(stage, src_of(x2 * nz + z2), dst_of(dx * nz + dz), (x2, z2, c, y))

    def arrived(stage, like):
        started.append((stage, like))
        pltpu.make_async_copy(like, like, recv.at[stage]).wait()

    def keep(src, dst, sem):
        copy = pltpu.make_async_copy(src, dst, sem)
        copy.start()
        return copy

    barrier = pltpu.get_barrier_semaphore()
    for dc, dy in hpeers:
        c2, y2 = hdev(dc, dy)
        pl.semaphore_signal(barrier, inc=1, device_id=(x, z, c2, y2), device_id_type=MESH)
    for dx, dz in gpeers:
        x2, z2 = gdev(dx, dz)
        pl.semaphore_signal(barrier, inc=1, device_id=(x2, z2, c, y), device_id_type=MESH)

    fetched = [
        keep(src, dst, loc_sem.at[5 + k])
        for k, (src, dst) in enumerate(
            [
                (traits_hbm, traits_ref),
                (mean_hbm, mean_ref),
                (firm_hbm, firm_ref),
                (order_row_hbm, order_row_ref),
                (weight_hbm, weight_ref),
                (loy_hbm, loy_ref),
                (share_hbm, share_ref),
                (scale_hbm, scale_ref),
                (size_hbm, size_ref),
                (order_hbm, order_ref),
            ]
        )
    ]
    get_draws = keep(draws_hbm, shock_own.at[pl.ds(0, ntraits)], loc_sem.at[0])
    get_share = keep(fshare_hbm.at[:, lanes(h)], fshare, loc_sem.at[1])

    lane = lax.broadcasted_iota(jnp.int32, (8, 128), 1)
    lane_jb, lane_m = lane // mdev, lax.rem(lane, mdev)
    lane16 = lax.broadcasted_iota(jnp.int32, (mdev, 128), 1)
    market = lax.broadcasted_iota(jnp.int32, (mdev, 128), 0)

    for copy in fetched:
        copy.wait()
    square[...] = jnp.zeros(square.shape, F32)
    for k in range(ntraits):
        square[k * mdev : (k + 1) * mdev, 0:64] = traits_ref[k] * (scale_ref[k] * LOG2E)
    mean_2 = mean_ref[...] * LOG2E
    mean_a = mean_2.astype(BF16).astype(F32)
    ids = firm_ref[...].astype(F32) - 256.0
    square[5 * mdev : 6 * mdev, 0:64] = mean_a
    square[6 * mdev : 7 * mdev, 0:64] = ids
    square[7 * mdev : 8 * mdev, 0:64] = mean_2 - mean_a
    pk_own[0:64, :] = square[...].T[0:64, :]
    for p in range(mdev // 2):
        even = square[6 * mdev + 2 * p : 6 * mdev + 2 * p + 1, :]
        odd = square[6 * mdev + 2 * p + 1 : 6 * mdev + 2 * p + 2, :]
        pk_own[64 + p : 65 + p, :] = even + pltpu.roll(odd, 64, 1)

    row_mass = None
    for m in range(mdev):
        shock_own[ntraits, m : m + 1, :] = weight_ref[m : m + 1, :] * size_ref[m]
    row_mass = jnp.sum(shock_own[ntraits], axis=1, keepdims=True)
    denom = jnp.sum(
        jnp.where(lax.rem(lane16, mdev) == market, row_mass, 0.0), axis=0, keepdims=True
    )

    order_f = order_row_ref[...].astype(F32) - 256.0
    for b in range(firms // 128):
        row = order_f[:, b * 128 : (b + 1) * 128]
        order_row_b[b] = jnp.broadcast_to(row, (16, 128)).astype(BF16)
        order_col_b[b * 128 : (b + 1) * 128, :] = jnp.broadcast_to(row, (128, 128)).T.astype(BF16)
    lane_b = lax.rem(lax.broadcasted_iota(jnp.int32, (16, 128), 1), mdev)
    for m in range(mdev):
        lane_mask[m] = jnp.where(lane_b == m, 1.0, 0.0).astype(BF16)
    kind = lax.rem(lax.broadcasted_iota(jnp.int32, (256, 128), 0) // mdev, 8)
    is_mean = jnp.logical_or(kind == 5, kind == 7)
    shocks_r[0] = jnp.where(is_mean, 1.0, 0.0).astype(BF16)
    shocks_r[1] = jnp.zeros((256, 128), BF16)

    def joined(ref):
        return jnp.concatenate([ref[k] for k in range(ref.shape[0])], axis=1)

    def folded(both):
        return both[:, :128] + both[:, 128:]

    def build(i, carry, forward=None):
        hh = source(i)
        pltpu.make_async_copy(pk.at[hh], pk.at[hh], recv_pk.at[i]).wait()
        if forward is not None:
            partner = (x, z, lax.rem(c + 1, nc), y)

            @pl.when(forward)
            def _():
                push(PK, pk.at[hh], pk.at[hh], partner, recv_pk.at[i + 1])

        base = pl.multiple_of(hh * mrows, mrows)
        one = jnp.ones((16, 128), BF16)
        zero = jnp.zeros((16, 128), BF16)
        for m in range(mdev):
            at = 6 * mdev + m
            for b in range(4):
                col = jnp.broadcast_to(pk[hh, b * 16 : b * 16 + 16, at : at + 1], (16, 128))
                col = col.astype(BF16)
                where = pl.ds(pl.multiple_of(base + m * 64 + b * 16, 16), 16)
                for t in range(firms // 128):
                    onehot[t, where, :] = jnp.where(col == order_row_b[t], one, zero)
        for p in range(mdev // 2):
            row = jnp.broadcast_to(pk[hh, 64 + p : 65 + p, :], (16, 128)).astype(BF16)
            for t in range(firms // 16):
                at = t * 16
                hot = jnp.where(order_col_b[at : at + 16, :] == row, one, zero)
                onehot_t[hh, p, at : at + 16, :] = hot
        return carry

    def tastes(i, carry):
        hh = source(i)
        pltpu.make_async_copy(shock.at[hh], shock.at[hh], recv_shock.at[i]).wait()
        hi, lo = split_hi_lo(shock[hh, 0:ntraits].reshape(ntraits * mdev, 128))
        for part_of in range(2):
            at = part_of * 128
            shocks_r[0, at : at + ntraits * mdev, :] = hi
            shocks_r[1, at : at + ntraits * mdev, :] = lo
        hi, lo = split_hi_lo(pk[hh, 0:64, :])
        for m in range(mdev):
            mask = lane_mask[m]
            for b in range(4):
                at = m * 64 + b * 16
                traits_l[0, at : at + 16, :] = hi[b * 16 : b * 16 + 16] * mask
                traits_l[1, at : at + 16, :] = lo[b * 16 : b * 16 + 16] * mask
        base = pl.multiple_of(hh * mrows, mrows)
        both = jnp.dot(joined(traits_l), joined(shocks_r), preferred_element_type=F32)
        util[pl.ds(base, mrows), :] = folded(both)
        return carry

    def set_terms(source):
        hi, lo = split_hi_lo(source[...].reshape(firms, 128) * LOG2E)
        terms[0] = hi
        terms[1] = lo

    def gather():
        chunk = nh * mrows // 2

        def block(q, carry):
            where = pl.ds(pl.multiple_of(q * chunk, chunk), chunk)
            hot = jnp.concatenate([onehot[t, where, :] for t in range(firms // 128)], axis=1)
            both = jnp.dot(hot, joined(terms), preferred_element_type=F32)
            gsum[where, :] = folded(both)
            return carry

        lax.fori_loop(0, 2, block, 0)

    keep(pk_own, pk.at[h], recv_pk.at[0])
    get_draws.wait()
    keep(shock_own.at[:, :, lanes(h)], shock.at[h], recv_shock.at[0])
    build(0, 0)

    pl.semaphore_wait(barrier, len(hpeers) + len(gpeers))

    to_h(LOY, lambda h2: loy_ref.at[:, lanes(h2)], loy_in.at[h])
    keep_loy = keep(loy_ref.at[:, lanes(h)], loy_in.at[h], loc_sem.at[2])
    to_h(PK, lambda h2: pk_own, pk.at[h], recv_pk, lambda dc, dy: dc == 0 or dy == 0)
    to_h(SHOCK, lambda h2: shock_own.at[:, :, lanes(h2)], shock.at[h], recv_shock)
    started.append((PK, pk.at[pl.ds(0, nh - 1)]))
    started.append((SHOCK, shock.at[pl.ds(0, nh - 1)]))

    square[0:mdev, 0:64] = share_ref[...]
    turned = square[...].T
    log_share = jnp.zeros((8, 128), F32)
    for jb in range(8):
        block = turned[jb * 8 : jb * 8 + 8, :]
        if jb:
            block = pltpu.roll(block, jb * mdev, 1)
        log_share = jnp.where(lane // mdev == jb, block, log_share)
    log_share = jnp.log(log_share)
    get_share.wait()
    for k in range(rows):
        fs_own[k : k + 1, :] = fshare[pl.ds(order_ref[g * rows + k], 1), :]
    fs_own[...] = jnp.log(fs_own[...])
    tastes(0, 0)
    build(1, 0)

    keep_loy.wait()
    arrived(LOY, loy_in.at[pl.ds(0, nh - 1)])
    for hh in range(nh):
        own_table[hh * own : (hh + 1) * own, :] = loy_in[hh]
    to_g(TABLE, lambda g2: own_table, lambda slot: table.at[g])
    keep_own = keep(own_table, table.at[g], loc_sem.at[3])

    others = ny - 1

    def build_next(k, carry):
        return build(2 + 2 * k - (2 * others - 1) * (k // others), carry, k < others)

    lax.fori_loop(0, nh - 2, build_next, 0)
    lax.fori_loop(1, nh, tastes, 0)
    keep_own.wait()
    arrived(TABLE, table.at[pl.ds(0, ng - 1)])
    set_terms(table)
    gather()
    tm = jnp.sum(shock[:, ntraits].reshape(nh * mdev, 128), axis=0, keepdims=True)
    tmass_s[...] = tm
    to_g(TMASS, lambda g2: tmass_s, lambda slot: tmass_r.at[slot])

    delta_sum = jnp.zeros((8, 128), F32)
    type_mass = None
    clip = None

    def clip_of(step):
        sq = jnp.sum(jnp.sum(sq2_r[step], axis=0), axis=1, keepdims=True)
        return jnp.minimum(1.0, CLIP_TARGET / jnp.sqrt(sq / (firms * draws_all) + NORM_EPS))

    own_new = own_table[...]

    for step in range(ITERS):
        stage = PER_STEP + STEP_STAGES * step

        if step:
            before = stage - STEP_STAGES
            arrived(before + SQ_H, sq2_r.at[step - 1, pl.ds(0, nh - 1)])
            clip = clip_of(step - 1)
            own_new = own_new + clip * gap

        def choices(hh, weighted, step=step, clip=clip):
            base = pl.multiple_of(hh * mrows, mrows)
            compact = jnp.zeros((8, 128), F32)
            for m in range(mdev):
                expu = []
                total = None
                for jb in range(8):
                    where = pl.ds(pl.multiple_of(base + m * 64 + jb * 8, 8), 8)
                    moved = gsum[where, :]
                    u = util[where, :] + (clip * moved if step else moved)
                    if step < ITERS - 1:
                        util[where, :] = u
                    e = jnp.exp2(u)
                    expu.append(e)
                    total = e if total is None else total + e
                total = jnp.sum(total, axis=0, keepdims=True)
                scale = shock[hh, ntraits, m : m + 1, :] / (1.0 + total)
                reds = None
                for jb in range(0, 8, 2):
                    at = m * 64 + jb * 8
                    wts = [expu[jb] * scale, expu[jb + 1] * scale]
                    for k in range(2):
                        red = jnp.sum(wts[k], axis=1, keepdims=True)
                        reds = red if reds is None else jnp.where(lane_jb == jb + k, red, reds)
                    hi, lo = split_hi_lo(jnp.concatenate(wts, axis=0))
                    weighted[0, at : at + 16, :] = hi
                    weighted[1, at : at + 16, :] = lo
                compact = jnp.where(lane_m == m, reds, compact)
            pred[step, hh] = compact

        def collected(hh, weighted):
            return jnp.dot(joined(onehot_t.at[hh]), joined(weighted), preferred_element_type=F32)

        def four_blocks(q, carry):
            sums = collected(jnp.maximum(4 * q - 1, 0), weighted[3])
            for k in range(4):
                choices(4 * q + k, weighted[k])
                if k < 3:
                    sums = sums + collected(4 * q + k, weighted[k])
            acc[...] = acc[...] + sums
            return carry

        acc[...] = jnp.zeros(acc.shape, F32)
        weighted[3][...] = jnp.zeros(weighted[3].shape, BF16)
        lax.fori_loop(0, nh // 4, four_blocks, 0)

        last = acc[...] + collected(nh - 1, weighted[3])
        part[step] = (last[:, :128] + last[:, 128:]).reshape(ng, rows, 128)
        to_g(stage + RS, lambda g2: part.at[step, g2], lambda slot: rs.at[step, slot - 1])
        to_h(stage + PRED, lambda h2: pred.at[step, h2], pred_r.at[step, h])

        arrived(stage + PRED, pred_r.at[step, pl.ds(0, nh - 1)])
        pred_r[step, h] = pred[step, h]
        num = jnp.sum(pred_r[step], axis=0)
        delta = log_share - jnp.log(num / denom)
        delta_sum = delta_sum + delta
        if step < ITERS - 1:
            dmean_s[step] = delta * LOG2E
            dmean[step, h] = delta * LOG2E
            to_h(stage + DMEAN, lambda h2: dmean_s.at[step], dmean.at[step, h])
        if step == 0:
            arrived(TMASS, tmass_r.at[pl.ds(1, ng - 1)])
            type_mass = tmass_s[...]
            for slot in range(1, ng):
                type_mass = type_mass + tmass_r[slot]

        arrived(stage + RS, rs.at[step])
        totals = part[step, g]
        for slot in range(ng - 1):
            totals = totals + rs[step, slot]
        gap = fs_own[...] - jnp.log(totals / type_mass)
        sq = jnp.sum(gap * gap, axis=0, keepdims=True)
        sq_s[step] = sq
        sq_r[step, 0] = sq
        to_g(stage + SQ_G, lambda g2: sq_s.at[step], lambda slot: sq_r.at[step, slot])
        if step < ITERS - 1:
            gap_s[step] = gap
            ag[step, g] = gap
            to_g(stage + AG, lambda g2: gap_s.at[step], lambda slot: ag.at[step, g])
            arrived(stage + DMEAN, dmean.at[step, pl.ds(0, nh - 1)])

            def shift(hh, carry, step=step):
                base = pl.multiple_of(hh * mrows, mrows)
                cols = dmean[step, hh]
                for m in range(mdev):
                    for jb in range(8):
                        where = pl.ds(pl.multiple_of(base + m * 64 + jb * 8, 8), 8)
                        at = jb * mdev + m
                        util[where, :] = util[where, :] + cols[:, at : at + 1]
                return carry

            lax.fori_loop(0, nh, shift, 0)
        else:
            for hh in range(nh):
                fin_s[hh, 0] = own_new[hh * own : (hh + 1) * own, :]
                fin_s[hh, 1] = gap[hh * own : (hh + 1) * own, :]
            to_h(OUT, lambda h2: fin_s.at[h2], fin.at[h])
            keep_out = keep(fin_s.at[h], fin.at[h], loc_sem.at[4])
            square[0:8, :] = delta_sum
            turned = square[...].T
            natural = jnp.zeros((mdev, 128), F32)
            for jb in range(8):
                block = turned[jb * mdev : (jb + 1) * mdev, :]
                if jb:
                    block = pltpu.roll(block, jb * 8, 1)
                natural = jnp.where(lane16 // 8 == jb, block, natural)
            mean_out[...] = mean_ref[...] + natural[:, 0:64]
        arrived(stage + SQ_G, sq_r.at[step, pl.ds(1, ng - 1)])
        sq = jnp.sum(sq_r[step], axis=0)
        sq2_s[step] = sq
        sq2_r[step, h] = sq
        to_h(stage + SQ_H, lambda h2: sq2_s.at[step], sq2_r.at[step, h])
        if step < ITERS - 1:
            arrived(stage + AG, ag.at[step, pl.ds(0, ng - 1)])
            set_terms(ag.at[step])
            gather()

    keep_out.wait()
    arrived(OUT, fin.at[pl.ds(0, nh - 1)])
    stage = PER_STEP + STEP_STAGES * (ITERS - 1)
    for at, like in started:
        pltpu.make_async_copy(like, like, send.at[at]).wait()
    arrived(stage + SQ_H, sq2_r.at[ITERS - 1, pl.ds(0, nh - 1)])
    clip = clip_of(ITERS - 1)
    for hh in range(nh):
        loy_out[:, hh * 128 : (hh + 1) * 128] = fin[hh, 0] + clip * fin[hh, 1]
    like = sq2_r.at[ITERS - 1, pl.ds(0, nh - 1)]
    pltpu.make_async_copy(like, like, send.at[stage + SQ_H]).wait()


def handed_on(mean_ref, loy_ref, mean_out, loy_out):
    mean_out[...] = mean_ref[...]
    loy_out[...] = loy_ref[...]


def local(
    mean_utility,
    market_share,
    product_traits,
    taste_draws,
    taste_scale,
    type_weight,
    market_size,
    product_firm,
    firm_order,
    loyalty,
    firm_share,
    shape,
):
    nx, nz, nc, ny = shape
    nh, ng = nc * ny, nx * nz
    mdev, ntraits, draws_all = taste_draws.shape
    firms = firm_share.shape[0]
    own = loyalty.shape[0]
    rows = firms // ng
    dims = (nx, nz, nc, ny, mdev, ntraits, firms, draws_all, own)
    vmem = pl.BlockSpec(memory_space=pltpu.VMEM)
    anywhere = pl.BlockSpec(memory_space=pl.ANY)
    scratch = [
        ((mdev, 64), F32),
        ((mdev, 64), F32),
        ((mdev, 64), jnp.int32),
        ((ntraits, mdev, 64), F32),
        ((mdev, draws_all), F32),
        ((own, draws_all), F32),
        ((1, firms), jnp.int32),
        ((128, 128), F32),
        ((72, 128), F32),
        ((nh, 72, 128), F32),
        ((ntraits + 1, mdev, draws_all), F32),
        ((nh, ntraits + 1, mdev, 128), F32),
        ((firms, 128), F32),
        ((rows, 128), F32),
        ((firms // 128, 16, 128), BF16),
        ((firms, 128), BF16),
        ((nh, own, 128), F32),
        ((rows, 128), F32),
        ((ng, rows, 128), F32),
        ((1, 128), F32),
        ((ng, 1, 128), F32),
        ((mdev, 16, 128), BF16),
        ((2, mdev * 64, 128), BF16),
        ((2, 256, 128), BF16),
        ((firms // 128, nh * mdev * 64, 128), BF16),
        ((nh, mdev // 2, firms, 128), BF16),
        ((nh * mdev * 64, 128), F32),
        ((nh * mdev * 64, 128), F32),
        ((2, mdev * 64, 128), BF16),
        ((2, mdev * 64, 128), BF16),
        ((2, mdev * 64, 128), BF16),
        ((2, mdev * 64, 128), BF16),
        ((2, firms, 128), BF16),
        ((firms, 256), F32),
        ((ITERS, ng, rows, 128), F32),
        ((ITERS, ng - 1, rows, 128), F32),
        ((ITERS, nh, 8, 128), F32),
        ((ITERS, nh, 8, 128), F32),
        ((ITERS - 1, nh, 8, 128), F32),
        ((ITERS - 1, 8, 128), F32),
        ((ITERS - 1, rows, 128), F32),
        ((ITERS - 1, ng, rows, 128), F32),
        ((ITERS, 1, 128), F32),
        ((ITERS, ng, 1, 128), F32),
        ((ITERS, 1, 128), F32),
        ((ITERS, nh, 1, 128), F32),
        ((nh, 2, own, 128), F32),
        ((nh, 2, own, 128), F32),
    ]
    stages = PER_STEP + STEP_STAGES * ITERS
    results = pl.pallas_call(
        functools.partial(kernel, dims),
        name="contraction",
        out_shape=(
            jax.ShapeDtypeStruct((mdev, 64), F32),
            jax.ShapeDtypeStruct((own, draws_all), F32),
        ),
        in_specs=[anywhere] * 12,
        out_specs=(vmem, vmem),
        scratch_shapes=[pltpu.VMEM(s, d) for s, d in scratch[:7]]
        + [
            pltpu.SMEM((ntraits,), F32),
            pltpu.SMEM((mdev,), F32),
            pltpu.SMEM((firms,), jnp.int32),
        ]
        + [pltpu.VMEM(s, d) for s, d in scratch[7:]]
        + [
            pltpu.SemaphoreType.DMA((15,)),
            pltpu.SemaphoreType.DMA((stages,)),
            pltpu.SemaphoreType.DMA((stages,)),
            pltpu.SemaphoreType.DMA((nh,)),
            pltpu.SemaphoreType.DMA((nh,)),
        ],
        compiler_params=pltpu.CompilerParams(
            collective_id=0, has_side_effects=True, vmem_limit_bytes=60 * 1024 * 1024
        ),
    )(
        mean_utility,
        market_share,
        product_firm,
        product_traits.transpose(2, 0, 1),
        taste_scale,
        market_size,
        type_weight,
        loyalty,
        firm_order,
        firm_order.reshape(1, firms),
        taste_draws.transpose(1, 0, 2),
        firm_share,
    )
    return pl.pallas_call(
        handed_on,
        name="handed_on",
        out_shape=tuple(jax.ShapeDtypeStruct(r.shape, F32) for r in results),
        in_specs=[vmem, vmem],
        out_specs=(vmem, vmem),
    )(*results)


def solution(mesh):
    shape = (4, 4, 2, mesh.shape["grp"])
    torus = Mesh(mesh.devices.reshape(shape), AXES)
    in_specs = (
        P(AXES, None),
        P(AXES, None),
        P(AXES, None, None),
        P(AXES, None, None),
        P(),
        P(AXES, None),
        P(AXES),
        P(AXES, None),
        P(),
        P(AXES, None),
        P(),
    )
    out_specs = (P(AXES, None), P(AXES, None))
    return jax.shard_map(
        functools.partial(local, shape=shape),
        mesh=torus,
        in_specs=in_specs,
        out_specs=out_specs,
        check_vma=False,
    )
```
